128 devices in a mesh: gx: 16 (over z, x), gy: 8 (over y, core).
Axes of the slice: x: 4, y: 4, z: 4, core: 2. Of those that a mesh axis runs over, the one named last changes fastest.
Arguments:
- displacement_old: float32 [3, 128, 128, 256], P(None, 'gx', 'gy'), may hold values from -6 to 6
- pressure_old: float32 [128, 128, 256], P('gx', 'gy'), may hold values from -6 to 6
- body_force: float32 [3, 128, 128, 256], P(None, 'gx', 'gy'), may hold values from -400 to 400
- fluid_source: float32 [128, 128, 256], P('gx', 'gy'), may hold values from -400 to 400
- material_ids: int32 [128, 128, 256], P('gx', 'gy'), may hold values from 0 to 7
- materials: float32 [5, 8], replicated, may hold values from 0.5 to 4
Outputs:
- displacement: float32 [3, 128, 128, 256], P(None, 'gx', 'gy')
- pressure: float32 [128, 128, 256], P('gx', 'gy')
The draws below stay inside these ranges and needn't reach their ends.
All inputs are finite; a program needn't handle non-finite values.
Results may differ from the reference program's by a relative error of at most 0.00017.
Values sent between devices are 32-bit elements; how exact they have to be, the bound alone decides.
No kernel may reach another device: no remote copies, remote signals or barrier semaphores. Data moves between devices by JAX's collectives and lax.ppermute only.
A program may use at most 64 MiB of HBM per device.

```python
import math
import jax
import jax.numpy as jnp
from jax import lax

NZ = 256
NMAT = 8
OUTER = 2
INNER = 3
NX = 128
NY = 128


def field_scale(key):
    key_rise, key_across = jax.random.split(key)
    planes = jnp.arange(NX, dtype=jnp.float32) / NX
    rising = 10.0 ** planes * jnp.exp(jax.random.uniform(key_rise, (NX,), minval=-0.35, maxval=0.35))
    across = jnp.exp(jax.random.uniform(key_across, (NY,), minval=-1.2, maxval=1.2))
    return rising[:, None, None] * across[None, :, None]


def rough_field(key, shape):
    key_scale, key_values = jax.random.split(jax.random.fold_in(key, 17))
    scale = field_scale(key_scale)
    values = jnp.clip(jax.random.normal(key_values, shape, jnp.float32), -6.0, 6.0)
    return (values * scale).astype(jnp.float32)


def draw_body_force(key, part):
    return rough_field(jax.random.fold_in(key, 101), (3, NX, NY, NZ))


def draw_fluid_source(key, part):
    return rough_field(jax.random.fold_in(key, 202), (NX, NY, NZ))


def plant(values, stream_key, low, top_value):
    spot = [jax.random.randint(jax.random.fold_in(stream_key, axis), (), 0, length) for axis, length in enumerate(values.shape)]
    main_axis = values.shape.index(max(values.shape))
    beside = spot[:main_axis] + [(spot[main_axis] + 1) % values.shape[main_axis]] + spot[main_axis + 1:]
    return values.at[tuple(spot)].set(low).at[tuple(beside)].set(top_value)


def block_levels(rng, extent, pieces, least, largest):
    factor_of, own = 1.0, jax.random.fold_in(rng, 6)
    for axis_at, shards_of in pieces:
        draws = jnp.exp(jax.random.uniform(jax.random.fold_in(own, axis_at), (shards_of,), jnp.float32, least / len(pieces), largest / len(pieces)))
        factor_of = factor_of * jnp.repeat(draws, extent[axis_at] // shards_of).reshape([-1 if axis == axis_at else 1 for axis in range(len(extent))])
    return factor_of


def normal_values(own_key, dims, spread, limit, pieces=(), kind=jnp.bfloat16):
    gain = block_levels(own_key, dims, pieces, -0.22, 0.18) if pieces else 1.0
    result = jax.random.normal(own_key, dims, jnp.float32) * spread * gain
    return jnp.minimum(jnp.maximum(result, -limit), limit).astype(kind)


def setup_inputs(seed: int = 0) -> dict:
    keys = jax.random.split(jax.random.key(seed), 7)
    return {
        "displacement_old": normal_values(keys[0], (3, NX, NY, NZ), 1.0, 6.0, ((1, 16), (2, 8)), jnp.float32),
        "pressure_old": normal_values(keys[1], (NX, NY, NZ), 1.0, 6.0, ((0, 16), (1, 8)), jnp.float32),
        "body_force": draw_body_force(jax.random.fold_in(keys[6], 71), 0),
        "fluid_source": draw_fluid_source(jax.random.fold_in(keys[6], 71), 0),
        "material_ids": plant(jax.random.randint(keys[4], (NX, NY, NZ), 0, NMAT), jax.random.fold_in(keys[4], 1), 0, NMAT - 1).astype(jnp.int32),
        "materials": jnp.clip(jnp.exp(jax.random.uniform(keys[5], (5, NMAT), jnp.float32, math.log(0.5), math.log(4.0))), 0.5, 4.0),
    }


step_time = 4.0


def shift_up(values, spatial):
    length = values.shape[spatial]
    widths = [(0, 0)] * values.ndim
    widths[spatial] = (0, 1)
    return lax.slice_in_dim(jnp.pad(values, widths), 1, length + 1, axis=spatial)


def shift_down(values, spatial):
    length = values.shape[spatial]
    widths = [(0, 0)] * values.ndim
    widths[spatial] = (1, 0)
    return lax.slice_in_dim(jnp.pad(values, widths), 0, length, axis=spatial)


def harmonic(first_value, second_value):
    return 2.0 * first_value * second_value / (first_value + second_value)


def divergence(field):
    return (shift_up(field[0], 0) - field[0] + shift_up(field[1], 1) - field[1]
            + shift_up(field[2], 2) - field[2])


def solve(operate, precond, rhs_vec, initial):
    solution = initial
    residual = rhs_vec - operate(initial)
    smoothed = precond(residual)
    direction = smoothed
    current = jnp.sum(residual * smoothed)
    for inner_step in range(INNER):
        image_vec = operate(direction)
        step_length = current / jnp.sum(direction * image_vec)
        solution = solution + step_length * direction
        if inner_step + 1 < INNER:
            residual = residual - step_length * image_vec
            smoothed = precond(residual)
            following = jnp.sum(residual * smoothed)
            direction = smoothed + (following / current) * direction
            current = following
    return solution


def reference(displacement_old, pressure_old, body_force, fluid_source, material_ids, materials):
    lame_first = materials[0][material_ids]
    shear_mod = materials[1][material_ids]
    permeability = materials[2][material_ids]
    storage = materials[3][material_ids]
    biot_coef = 0.25 * materials[4][material_ids]
    stiff_up = [0.5 * (shear_mod + shift_up(shear_mod, spatial)) for spatial in range(3)]
    stiff_down = [0.5 * (shear_mod + shift_down(shear_mod, spatial)) for spatial in range(3)]
    flow_up = [harmonic(permeability, shift_up(permeability, spatial)) for spatial in range(3)]
    flow_down = [harmonic(permeability, shift_down(permeability, spatial)) for spatial in range(3)]
    stab = biot_coef * biot_coef / (lame_first + (2.0 / 3.0) * shear_mod)
    storage_total = storage + stab
    flow_sum = flow_up[0] + flow_down[0] + flow_up[1] + flow_down[1] + flow_up[2] + flow_down[2]
    inv_pressure = 1.0 / (storage_total + step_time * flow_sum)
    stiff_sum = stiff_up[0] + stiff_down[0] + stiff_up[1] + stiff_down[1] + stiff_up[2] + stiff_down[2]
    inv_blocks = 1.0 / jnp.stack([stiff_sum + shift_down(lame_first, spatial) for spatial in range(3)])
    factor = lame_first / (1.0 + lame_first * (inv_blocks[0] + inv_blocks[1] + inv_blocks[2]))

    def apply_pressure(field):
        flux = jnp.zeros_like(field)
        for spatial in range(3):
            flux = (flux + flow_up[spatial] * (field - shift_up(field, spatial))
                    + flow_down[spatial] * (field - shift_down(field, spatial)))
        return storage_total * field + step_time * flux

    def apply_mech(field):
        summed = jnp.zeros_like(field)
        for spatial in range(3):
            summed = (summed + stiff_up[spatial] * (field - shift_up(field, spatial + 1))
                      + stiff_down[spatial] * (field - shift_down(field, spatial + 1)))
        weighted = lame_first * divergence(field)
        lame_pull = jnp.stack([shift_down(weighted, spatial) - weighted for spatial in range(3)])
        return summed + lame_pull

    def solve_pressure(residual):
        return residual * inv_pressure

    def solve_blocks(residual):
        scaled = residual * inv_blocks
        summed = scaled[0] + scaled[1] + scaled[2]
        return scaled - inv_blocks * (factor * summed)

    pressure = pressure_old
    displacement = displacement_old
    for repeat in range(OUTER):
        change = displacement - displacement_old
        rhs_pressure = (storage * pressure_old + step_time * fluid_source
                        - biot_coef * divergence(change) + stab * pressure)
        pressure = solve(apply_pressure, solve_pressure, rhs_pressure, pressure)
        loaded = biot_coef * pressure
        pressure_push = jnp.stack([shift_down(loaded, spatial) - loaded for spatial in range(3)])
        rhs_mech = body_force + pressure_push
        displacement = solve(apply_mech, solve_blocks, rhs_mech, displacement)
    return displacement, pressure
```

```python
import functools

import jax
import jax.numpy as jnp
from jax import lax
from jax.experimental import pallas as pl
from jax.experimental.pallas import tpu as pltpu
from jax.sharding import PartitionSpec as P

F32 = jnp.float32
DT = 4.0
TAU_U = -0.45
TAU_P = 0.0
NX, NY, NZ = 8, 16, 256
YE = 32
LOW, HIGH = 7, 6
XE = LOW + NX + HIGH
ML = 4
ME = NX + 2 * ML
MO = LOW - ML
PIVOT = 2e-7
VMEM_LIMIT = 48 * 1024 * 1024

VM = pl.BlockSpec(memory_space=pltpu.VMEM)
SM = pl.BlockSpec(memory_space=pltpu.SMEM)


def up_y(v):
    return pltpu.roll(v, v.shape[0] - 1, 0)


def dn_y(v):
    return pltpu.roll(v, 1, 0)


def up_z(v):
    return pltpu.roll(v, v.shape[1] - 1, 1)


def dn_z(v):
    return pltpu.roll(v, 1, 1)


def lane():
    return lax.broadcasted_iota(jnp.int32, (YE, NZ), 1)


def loop(low, high, body, unroll=1):
    def step(x, carry):
        body(x)
        return carry

    lax.fori_loop(low, high, step, 0, unroll=unroll)


def lookup(code, mats, rows):
    found = [jnp.zeros(code.shape, F32) for _ in rows]
    for m in range(8):
        hit = code == float(m + 1)
        found = [jnp.where(hit, mats[r, m], v) for r, v in zip(rows, found)]
    return found


def pack_x_kernel(ids, p, f, u, b, up, dn):
    k = 0
    for x in range(1, 8):
        up[k] = (ids[x] + 1).astype(F32)
        up[7 + k] = p[x]
        k += 1
    up[14:20] = f[2:8]
    for a in range(3):
        up[20 + 4 * a : 24 + 4 * a] = u[a, 4:8]
        up[32 + 3 * a : 35 + 3 * a] = b[a, 5:8]
    for x in range(6):
        dn[x] = (ids[x] + 1).astype(F32)
    dn[6:12] = p[0:6]
    dn[12:17] = f[0:5]
    for a in range(3):
        dn[17 + 4 * a : 21 + 4 * a] = u[a, 0:4]
        dn[29 + 3 * a : 32 + 3 * a] = b[a, 0:3]


def pick(x, low, own, high, first, n_low):
    if x < n_low:
        return low, first[0] + x
    if x < n_low + NX:
        return own, x - n_low
    return high, first[1] + x - n_low - NX


def pack_y_kernel(ids, p, f, u, b, low, high, up, dn):
    for x in range(21):
        ref, i = pick(x, low, ids, high, (0, 0), 7)
        for out, rows in ((up, slice(8, 16)), (dn, slice(0, 8))):
            v = ref[i, rows]
            out[x] = (v + 1).astype(F32) if ref is ids else v
        ref, i = pick(x, low, p, high, (7, 6), 7)
        up[21 + x] = ref[i, 8:16]
        dn[21 + x] = ref[i, 0:8]
    for x in range(19):
        ref, i = pick(x, low, f, high, (14, 12), 6)
        up[42 + x] = ref[i, 8:16]
        dn[42 + x] = ref[i, 0:8]
    for a in range(3):
        for m in range(16):
            ref, i = pick(m, low, u.at[a], high, (20 + 4 * a, 17 + 4 * a), 4)
            k, r = 61 + 8 * a + m // 2, 4 * (m % 2)
            up[k, r : r + 4] = ref[i, 12:16]
            dn[k, r : r + 4] = ref[i, 0:4]
        for m in range(14):
            ref, i = pick(m, low, b.at[a], high, (32 + 3 * a, 29 + 3 * a), 3)
            k, r = 85 + 7 * a + m // 2, 4 * (m % 2)
            up[k, r : r + 4] = ref[i, 12:16]
            dn[k, r : r + 4] = ref[i, 0:4]


def fill(out, n, n_low, own, low, high, first, yl, yh, k, flags, cast=None):
    for x in range(n):
        ref, i = pick(x, low, own, high, first, n_low)
        v = ref[i]
        if cast is not None and ref is own:
            v = cast(v)
        lo, hi = (yl[k + x], yh[k + x])
        if flags is not None:
            if x < n_low:
                edge = flags[0]
            elif x >= n_low + NX:
                edge = flags[1]
            else:
                edge = None
            lo, hi = (lo * flags[2], hi * flags[3])
            if edge is not None:
                v, lo, hi = (v * edge, lo * edge, hi * edge)
        out[x, 8:24] = v
        out[x, 0:8] = lo
        out[x, 24:32] = hi


def fill_half(out, n, n_low, own, low, high, first, yl, yh, k, flags, offset=0):
    for x in range(n):
        ref, i = pick(x, low, own, high, first, n_low)
        v = ref[i]
        r = 4 * (x % 2)
        lo, hi = (yl[k + x // 2, r : r + 4], yh[k + x // 2, r : r + 4])
        if flags is not None:
            if x < n_low:
                edge = flags[0]
            elif x >= n_low + NX:
                edge = flags[1]
            else:
                edge = None
            lo, hi = (lo * flags[2], hi * flags[3])
            if edge is not None:
                v, lo, hi = (v * edge, lo * edge, hi * edge)
        zero = jnp.zeros((4, NZ), F32)
        out[x + offset, 8:24] = v
        out[x + offset, 0:4] = zero
        out[x + offset, 4:8] = lo
        out[x + offset, 24:28] = hi
        out[x + offset, 28:32] = zero


def spread(parts, out):
    at = lax.broadcasted_iota(jnp.int32, (8, 128), 1)
    row = jnp.zeros((8, 128), F32)
    for k, part in enumerate(parts):
        row = jnp.where(at == k, jnp.sum(part), row)
    for i in range(0, 128, 8):
        out[i : i + 8] = row


def moments(left, right, last, out, comps, first):
    def body(x, acc):
        acc = list(acc)
        for a in range(comps):
            s = [v[a, first + x, 8:24] for v in left]
            q = [v[a, first + x, 8:24] for v in right]
            terms = (s[0] * q[0], s[0] * q[1], s[1] * q[1], s[1] * q[2], s[2] * q[2], s[2] * q[3])
            acc = [t + w for t, w in zip(acc, terms)]
        return tuple(acc)

    zero = jnp.zeros((NY, NZ), F32)
    spread(lax.fori_loop(0, NX, body, (zero,) * 6), out)


def coefficients(rows, tau):
    total = jnp.sum(rows[...], axis=0, keepdims=True)
    mu = [jnp.broadcast_to(total[:, k : k + 1], (1, 128)) for k in range(6)]
    g = lambda i: (1.0 - tau) * mu[i] - mu[i + 1]
    g00, g01, g02, g12, g22 = g(0), g(1), g(2), g(3), g(4)
    g11 = g02
    inverse = lambda d, scale: jnp.where(d > PIVOT * scale, 1.0 / d, 0.0)
    i0 = inverse(g00, 0.0 * g00)
    l10, l20 = g01 * i0, g02 * i0
    i1 = inverse(g11 - l10 * g01, g11)
    e = g12 - l10 * g02
    l21 = e * i1
    i2 = inverse(g22 - l20 * g02 - l21 * e, g22)
    c0 = mu[0]
    c1 = mu[1] - l10 * c0
    c2 = mu[2] - l20 * c0 - l21 * c1
    y2 = c2 * i2
    y1 = c1 * i1 - l21 * y2
    y0 = c0 * i0 - l10 * y1 - l20 * y2
    return y0[0, 0], y1[0, 0], y2[0, 0]


def pressure_around(v, x, cx, cy, cz):
    c = v[x]
    y, z = cy[x], cz[x]
    return (
        cx[x] * v[x + 1]
        + cx[x - 1] * v[x - 1]
        + y * up_y(c)
        + dn_y(y * c)
        + z * up_z(c)
        + dn_z(z * c)
    )


def pressure_chain(start, p, cx, cy, cz, inv, t, n, part):
    def first(x):
        r = start(x) + pressure_around(p, x, cx, cy, cz)
        n[0, x] = r
        t[0, x] = inv[x] * r

    loop(1, XE - 1, first)
    for i in (1, 2):

        def follow(x):
            r = pressure_around(t.at[i - 1], x, cx, cy, cz)
            n[i, x] = r
            t[i, x] = inv[x] * r

        loop(1 + i, XE - 1 - i, follow)

    def final(x):
        n[3, x] = pressure_around(t.at[2], x, cx, cy, cz)

    loop(LOW, LOW + NX, final)
    moments([t.at[i : i + 1] for i in range(3)], [n.at[i : i + 1] for i in range(4)], None, part, 1, LOW)


def pressure_first_kernel(
    flags, mats, ids, p, f, low, high, yl, yh,
    code, pe, coef, t, part,
    fe, perm, stor, stab, n,
):
    cx, cy, cz, inv, diag, base, biot = (coef.at[i] for i in range(7))
    fill(code, XE, LOW, ids, low, high, (0, 0), yl, yh, 0, flags, lambda v: (v + 1).astype(F32))
    fill(pe, XE, LOW, p, low, high, (7, 6), yl, yh, 21, flags)
    fill(fe.at[1:20], XE - 2, LOW - 1, f, low, high, (14, 12), yl, yh, 42, None)

    def tables(x):
        l, s, k, st, bi = lookup(code[x], mats, range(5))
        bi = 0.25 * bi
        perm[x] = k
        stor[x] = st
        biot[x] = bi
        stab[x] = bi * bi / jnp.maximum(l + (2.0 / 3.0) * s, 1e-30)

    loop(0, XE, tables)

    def faces(x):
        k = perm[x]

        def harmonic(other):
            return (2.0 * DT) * k * other / jnp.maximum(k + other, 1e-30)

        cx[x] = harmonic(perm[x + 1])
        cy[x] = harmonic(up_y(k))
        cz[x] = jnp.where(lane() < NZ - 1, harmonic(up_z(k)), 0.0)

    loop(0, XE - 1, faces)

    def diagonal(x):
        y, z = cy[x], cz[x]
        flow = cx[x] + cx[x - 1] + y + dn_y(y) + z + dn_z(z)
        inside = code[x] > 0.5
        d = stor[x] + stab[x] + flow
        inv[x] = jnp.where(inside, 1.0 / jnp.where(inside, d, 1.0), 0.0)
        diag[x] = stab[x] - d
        base[x] = stor[x] * pe[x] + DT * fe[x]

    loop(1, XE - 1, diagonal)
    pressure_chain(lambda x: base[x] + diag[x] * pe[x], pe, cx, cy, cz, inv, t, n, part)


def pressure_next_kernel(
    flags, coef, p, du, uo, low, high, yl, yh,
    pe, ue, t, part,
    de, n,
):
    cx, cy, cz, inv, diag, base, biot = (coef.at[i] for i in range(7))
    for a in range(3):
        fill(de.at[a, 1:21], XE - 1, LOW - 1, du.at[a], low, high, (6 * a, 6 * a), yl, yh, 20 * a, flags)
    fill(pe, XE, LOW, p, low, high, (18, 18), yl, yh, 60, flags)

    def start(x):
        c2 = de[2, x]
        div = (
            de[0, x + 1] - de[0, x]
            + up_y(de[1, x]) - de[1, x]
            + jnp.where(lane() < NZ - 1, up_z(c2), 0.0) - c2
        )
        return base[x] - biot[x] * div + diag[x] * pe[x]

    pressure_chain(start, pe, cx, cy, cz, inv, t, n, part)

    def shifted(m):
        for a in range(3):
            ue[a, m] = uo[a, m] + de[a, m + MO]

    loop(0, ME, shifted)


def shear_around(w, m, sx, sy, sz):
    c = w[m]
    y, z = sy[m], sz[m]
    return (
        sx[m] * w[m + 1]
        + sx[m - 1] * w[m - 1]
        + y * up_y(c)
        + dn_y(y * c)
        + z * up_z(c)
        + dn_z(z * c)
    )


def mech_chain(u, bf, load, mc, s, q, carry, part):
    sx, sy, sz, diag, lame, h0, h1, h2, kk = (mc.at[i] for i in range(9))
    h = (h0, h1, h2)

    def ups(w, m):
        return (
            w[0, m + 1],
            up_y(w[1, m]),
            jnp.where(lane() < NZ - 1, up_z(w[2, m]), 0.0),
        )

    def precondition(r, m):
        scaled = [r[a] * h[a][m] for a in range(3)]
        g = kk[m] * (scaled[0] + scaled[1] + scaled[2])
        return [scaled[a] - h[a][m] * g for a in range(3)]

    def pull(m):
        p = ups(u, m)
        t = p[0] + p[1] + p[2]
        return load[m] - lame[m] * (t - (u[0, m] + u[1, m] + u[2, m]))

    carry[0] = pull(0)

    def first(m):
        c = pull(m)
        low = (carry[0], dn_y(c), jnp.where(lane() > 0, dn_z(c), 0.0))
        r = []
        for a in range(3):
            r.append(
                bf[a, m] + low[a] - c - diag[m] * u[a, m] + shear_around(u.at[a], m, sx, sy, sz)
            )
        carry[0] = c
        z = precondition(r, m)
        for a in range(3):
            q[0, a, m] = r[a]
            s[0, a, m] = z[a]

    loop(1, ME - 1, first)

    def image(w, m):
        p = ups(w, m)
        t = p[0] + p[1] + p[2]
        e = (w[0, m] + w[1, m] + w[2, m]) - t
        l = lame[m]
        low = (
            carry[0],
            dn_y(l * (p[1] + e)),
            jnp.where(lane() > 0, dn_z(l * (p[2] + e)), 0.0),
        )
        carry[0] = l * (p[0] + e)
        push = l * t
        return [
            shear_around(w.at[a], m, sx, sy, sz) + push + low[a] for a in range(3)
        ]

    def carry_in(w, m):
        p = ups(w, m)
        t = p[0] + p[1] + p[2]
        carry[0] = lame[m] * (p[0] + (w[0, m] + w[1, m] + w[2, m]) - t)

    for i in (1, 2):
        w = s.at[i - 1]
        carry_in(w, i)

        def follow(m):
            r = image(w, m)
            r = [r[a] - TAU_U * q[i - 1, a, m] for a in range(3)]
            z = precondition(r, m)
            for a in range(3):
                q[i, a, m] = r[a]
                s[i, a, m] = z[a]

        loop(1 + i, ME - 1 - i, follow)

    carry_in(s.at[2], ML - 1)

    def final(m):
        r = image(s.at[2], m)
        for a in range(3):
            q[3, a, m] = r[a] - TAU_U * q[2, a, m]

    loop(ML, ML + NX, final)
    moments([s.at[i] for i in range(3)], [q.at[i] for i in range(4)], None, part, 3, ML)


def update_pressure(rows, t, pe, biot_of, pout, load):
    y = coefficients(rows, TAU_P)

    def body(m):
        x = m + MO
        v = pe[x] + (y[0] * t[0, x] + y[1] * t[1, x] + y[2] * t[2, x])
        load[m] = biot_of(x) * v
        pout[m] = v

    loop(0, ME - 1, body)


def mech_first_kernel(
    flags, mats, rows, code, pe, coef, t, u, b, low, high, yl, yh,
    pnew, ue, be, mc, s, part,
    q, load, pm, shear, sall, carry,
):
    sx, sy, sz, diag, lame, h0, h1, h2, kk = (mc.at[i] for i in range(9))
    biot = coef.at[6]
    for a in range(3):
        fill_half(ue.at[a], 16, 4, u.at[a], low, high, (20 + 4 * a, 17 + 4 * a), yl, yh, 61 + 8 * a, flags)
        fill_half(be.at[a], 14, 3, b.at[a], low, high, (32 + 3 * a, 29 + 3 * a), yl, yh, 85 + 7 * a, None, 1)

    def tables(m):
        l, g = lookup(code[m + MO], mats, (0, 1))
        lame[m] = l
        shear[m] = g

    loop(0, ME, tables)

    def faces(m):
        g = shear[m]
        sx[m] = 0.5 * (g + shear[m + 1])
        sy[m] = 0.5 * (g + up_y(g))
        sz[m] = jnp.where(lane() < NZ - 1, 0.5 * (g + up_z(g)), 0.0)

    loop(0, ME - 1, faces)

    def diagonal(m):
        g, l = shear[m], lame[m]
        around = (
            shear[m + 1] + shear[m - 1] + up_y(g) + dn_y(g)
            + jnp.where(lane() < NZ - 1, up_z(g), 0.0)
            + jnp.where(lane() > 0, dn_z(g), 0.0)
        )
        d = 3.0 * g + 0.5 * around
        diag[m] = d
        inside = code[m + MO] > 0.5
        lows = (lame[m - 1], dn_y(l), jnp.where(lane() > 0, dn_z(l), 0.0))
        hs = [jnp.where(inside, 1.0 / jnp.where(inside, d + v, 1.0), 0.0) for v in lows]
        h0[m], h1[m], h2[m] = hs
        kk[m] = l / (1.0 + l * (hs[0] + hs[1] + hs[2]))

    loop(1, ME - 1, diagonal)
    update_pressure(rows, t, pe, lambda x: biot[x], pm, load)
    for x in range(NX):
        pnew[x] = pm[x + ML, 8:24]
    mech_chain(ue, be, load, mc, sall, q, carry, part)
    for i in range(3):
        for a in range(3):
            for x in range(NX):
                s[i, a, x] = sall[i, a, x + ML, 8:24]


def mech_next_kernel(
    rows, pe, coef, t, ue, be, mc,
    pnew, s, part,
    q, load, pm, sall, carry,
):
    biot = coef.at[6]
    update_pressure(rows, t, pe, lambda x: biot[x], pm, load)
    for x in range(NX):
        pnew[x] = pm[x + ML, 8:24]
    mech_chain(ue, be, load, mc, sall, q, carry, part)
    for i in range(3):
        for a in range(3):
            for x in range(NX):
                s[i, a, x] = sall[i, a, x + ML, 8:24]


def change_kernel(rows, s, u, p, du, unew, up, dn):
    y = coefficients(rows, TAU_U)
    for a in range(3):
        for x in range(NX):
            d = y[0] * s[0, a, x] + y[1] * s[1, a, x] + y[2] * s[2, a, x]
            du[a, x] = d
            unew[a, x] = u[a, x] + d
            if x >= 2:
                up[6 * a + x - 2] = d
            if x < 6:
                dn[6 * a + x] = d
    up[18:25] = p[1:8]
    dn[18:24] = p[0:6]


def pack_change_kernel(du, p, low, high, up, dn):
    for a in range(3):
        for x in range(20):
            ref, i = pick(x, low, du.at[a], high, (6 * a, 6 * a), 6)
            up[20 * a + x] = ref[i, 8:16]
            dn[20 * a + x] = ref[i, 0:8]
    for x in range(21):
        ref, i = pick(x, low, p, high, (18, 18), 7)
        up[60 + x] = ref[i, 8:16]
        dn[60 + x] = ref[i, 0:8]


def finish_kernel(rows, s, u, out):
    y = coefficients(rows, TAU_U)
    for a in range(3):
        for x in range(NX):
            out[a, x] = u[a, x] + (y[0] * s[0, a, x] + y[1] * s[1, a, x] + y[2] * s[2, a, x])


def call(kernel, name, ins, outs, scratch=(), specs=None):
    return pl.pallas_call(
        kernel,
        name=name,
        out_shape=[jax.ShapeDtypeStruct(o, F32) for o in outs],
        in_specs=specs or [VM] * len(ins),
        out_specs=[VM] * len(outs),
        scratch_shapes=[pltpu.VMEM(s, F32) for s in scratch],
        compiler_params=pltpu.CompilerParams(vmem_limit_bytes=VMEM_LIMIT),
    )(*ins)


def neighbours(axis, size, up, dn):
    ring = [(i, (i + 1) % size) for i in range(size)]
    return lax.ppermute(up, axis, ring), lax.ppermute(dn, axis, [(b, a) for a, b in ring])


def gather_rows(part):
    return lax.all_to_all(part, ("gx", "gy"), 0, 0, tiled=True)


def on_device(gx_size, gy_size, u, p, b, f, ids, mats):
    gx, gy = lax.axis_index("gx"), lax.axis_index("gy")
    flags = jnp.stack([gx > 0, gx < gx_size - 1, gy > 0, gy < gy_size - 1]).astype(F32)
    wide = (YE, NZ)
    up, dn = call(pack_x_kernel, "pack_x", (ids, p, f, u, b), [(41, NY, NZ), (38, NY, NZ)])
    low, high = neighbours("gx", gx_size, up, dn)
    up, dn = call(
        pack_y_kernel, "pack_y", (ids, p, f, u, b, low, high), [(106, 8, NZ), (106, 8, NZ)]
    )
    yl, yh = neighbours("gy", gy_size, up, dn)
    code, pe, coef, t, part = call(
        pressure_first_kernel,
        "pressure_first",
        (flags, mats, ids, p, f, low, high, yl, yh),
        [(XE, *wide), (XE, *wide), (7, XE, *wide), (3, XE, *wide), (128, 128)],
        [(XE, *wide)] * 4 + [(4, XE, *wide)],
        [SM, SM] + [VM] * 7,
    )
    rows = gather_rows(part)
    p1, ue, be, mc, s, part = call(
        mech_first_kernel,
        "mech_first",
        (flags, mats, rows, code, pe, coef, t, u, b, low, high, yl, yh),
        [(NX, NY, NZ), (3, ME, *wide), (3, ME, *wide), (9, ME, *wide), (3, 3, NX, NY, NZ), (128, 128)],
        [(4, 3, ME, *wide), (ME, *wide), (ME, *wide), (ME, *wide), (3, 3, ME, *wide), (1, *wide)],
        [SM, SM] + [VM] * 11,
    )
    rows = gather_rows(part)
    du, u1, up, dn = call(
        change_kernel,
        "change",
        (rows, s, u, p1),
        [(3, NX, NY, NZ), (3, NX, NY, NZ), (25, NY, NZ), (24, NY, NZ)],
    )
    low, high = neighbours("gx", gx_size, up, dn)
    up, dn = call(pack_change_kernel, "pack_change", (du, p1, low, high), [(81, 8, NZ), (81, 8, NZ)])
    yl, yh = neighbours("gy", gy_size, up, dn)
    pe, ue, t, part = call(
        pressure_next_kernel,
        "pressure_next",
        (flags, coef, p1, du, ue, low, high, yl, yh),
        [(XE, *wide), (3, ME, *wide), (3, XE, *wide), (128, 128)],
        [(3, XE, *wide), (4, XE, *wide)],
        [SM] + [VM] * 8,
    )
    rows = gather_rows(part)
    p2, s, part = call(
        mech_next_kernel,
        "mech_next",
        (rows, pe, coef, t, ue, be, mc),
        [(NX, NY, NZ), (3, 3, NX, NY, NZ), (128, 128)],
        [(4, 3, ME, *wide), (ME, *wide), (ME, *wide), (3, 3, ME, *wide), (1, *wide)],
    )
    rows = gather_rows(part)
    (u2,) = call(finish_kernel, "finish", (rows, s, u1), [(3, NX, NY, NZ)])
    return u2, p2


def solution(mesh):
    body = functools.partial(on_device, mesh.shape["gx"], mesh.shape["gy"])
    field, vector = P("gx", "gy", None), P(None, "gx", "gy", None)
    return jax.shard_map(
        body,
        mesh=mesh,
        in_specs=(vector, field, vector, field, field, P()),
        out_specs=(vector, field),
        check_vma=False,
    )
```

```python
import functools

import jax
import jax.numpy as jnp
from jax import lax
from jax.experimental import pallas as pl
from jax.experimental.pallas import tpu as pltpu
from jax.sharding import PartitionSpec as P

F32 = jnp.float32
DT = 4.0
NX, NY, NZ = 8, 16, 256
YE = 32
YM = 24
GENS = 4
PAIRS = [(a, b) for a in range(GENS) for b in range(a, GENS)]
LEVELS = ((0, 0), (0, 1), (1, 1), (1, 2), (2, 2), (2, 3))
LOW, HIGH = 7, 6
XE = LOW + NX + HIGH
ML = 4
ME = NX + 2 * ML
MO = LOW - ML
PK = ML + NX + 3
PIVOT = 2e-7
PW = 4
COST = 200_000_000

VM = pl.BlockSpec(memory_space=pltpu.VMEM)
SM = pl.BlockSpec(memory_space=pltpu.SMEM)
HB = pl.BlockSpec(memory_space=pltpu.HBM)


def up_y(v):
    return pltpu.roll(v, v.shape[0] - 1, 0)


def dn_y(v):
    return pltpu.roll(v, 1, 0)


def up_z(v):
    low, high = pltpu.roll(v[:, :128], 127, 1), pltpu.roll(v[:, 128:], 127, 1)
    inner = lax.broadcasted_iota(jnp.int32, low.shape, 1) < 127
    return jnp.concatenate([jnp.where(inner, low, high), jnp.where(inner, high, 0.0)], axis=1)


def dn_z(v):
    low, high = pltpu.roll(v[:, :128], 1, 1), pltpu.roll(v[:, 128:], 1, 1)
    inner = lax.broadcasted_iota(jnp.int32, low.shape, 1) > 0
    return jnp.concatenate([jnp.where(inner, low, 0.0), jnp.where(inner, high, low)], axis=1)


def loop(low, high, compute, width=1):
    def group(x, count):
        for i in range(count):
            for ref, index, value in compute(x + i):
                ref[index] = value

    steps = (high - low) // width

    def step(k, carry):
        group(low + k * width, width)
        return carry

    lax.fori_loop(0, steps, step, 0)
    if (high - low) % width:
        group(low + steps * width, (high - low) % width)


def lookup(code, mats, rows):
    found = [jnp.zeros(code.shape, F32) for _ in rows]
    for m in range(8):
        hit = code == float(m + 1)
        found = [jnp.where(hit, mats[r, m], v) for r, v in zip(rows, found)]
    return found


def pack_x_kernel(ids, p, f, u, b, up_p, dn_p, up_m, dn_m, code, pv, fv, raw, sems):
    copies = []

    def take(src, dst):
        copies.append(pltpu.make_async_copy(src, dst, sems.at[len(copies)]))
        copies[-1].start()

    take(ids, raw)
    take(p, pv)
    take(f, fv)
    take(p.at[1:8], up_p.at[7:14])
    take(p.at[0:6], dn_p.at[6:12])
    take(f.at[2:8], up_p.at[14:20])
    take(f.at[0:5], dn_p.at[12:17])
    for a in range(3):
        take(u.at[a, 4:8], up_m.at[4 * a : 4 * a + 4])
        take(u.at[a, 0:4], dn_m.at[4 * a : 4 * a + 4])
        take(b.at[a, 5:8], up_m.at[12 + 3 * a : 15 + 3 * a])
        take(b.at[a, 0:3], dn_m.at[12 + 3 * a : 15 + 3 * a])
    copies[0].wait()
    for x in range(NX):
        c = (raw[x] + 1).astype(F32)
        code[x] = c
        if x >= 1:
            up_p[x - 1] = c
        if x < 6:
            dn_p[x] = c
    for copy in copies[1:]:
        copy.wait()


def pick(x, low, own, high, first, n_low):
    if x < n_low:
        return low, first[0] + x
    if x < n_low + NX:
        return own, x - n_low
    return high, first[1] + x - n_low - NX


def pack_y_pressure_kernel(ids, p, f, low, high, up, dn):
    for x in range(21):
        ref, i = pick(x, low, ids, high, (0, 0), 7)
        up[x] = ref[i, 8:16]
        dn[x] = ref[i, 0:8]
        ref, i = pick(x, low, p, high, (7, 6), 7)
        up[21 + x] = ref[i, 8:16]
        dn[21 + x] = ref[i, 0:8]
    for x in range(19):
        ref, i = pick(x, low, f, high, (14, 12), 6)
        up[42 + x] = ref[i, 8:16]
        dn[42 + x] = ref[i, 0:8]


def pack_y_mech_kernel(u, b, low, high, up, dn):
    for a in range(3):
        for m in range(16):
            ref, i = pick(m, low, u.at[a], high, (4 * a, 4 * a), 4)
            k, r = 8 * a + m // 2, 4 * (m % 2)
            up[k, r : r + 4] = ref[i, 12:16]
            dn[k, r : r + 4] = ref[i, 0:4]
        for m in range(14):
            ref, i = pick(m, low, b.at[a], high, (12 + 3 * a, 12 + 3 * a), 3)
            k, r = 24 + 7 * a + m // 2, 4 * (m % 2)
            up[k, r : r + 4] = ref[i, 12:16]
            dn[k, r : r + 4] = ref[i, 0:4]


def masked(x, n_low, flags, v, lo, hi):
    if flags is None:
        return v, lo, hi
    lo, hi = (lo * flags[2], hi * flags[3])
    if n_low <= x < n_low + NX:
        return v, lo, hi
    edge = flags[0] if x < n_low else flags[1]
    return v * edge, lo * edge, hi * edge


def fill(out, n, n_low, own, low, high, first, yl, yh, k, flags):
    for x in range(n):
        ref, i = pick(x, low, own, high, first, n_low)
        v, lo, hi = masked(x, n_low, flags, ref[i], yl[k + x], yh[k + x])
        out[x, 8:24] = v
        out[x, 0:8] = lo
        out[x, 24:32] = hi


def fill_mech(out, n, n_low, own, low, high, first, yl, yh, k, flags, offset):
    for x in range(n):
        ref, i = pick(x, low, own, high, first, n_low)
        r = 4 * (x % 2)
        lo, hi = yl[k + x // 2, r : r + 4], yh[k + x // 2, r : r + 4]
        v, lo, hi = masked(x, n_low, flags, ref[i], lo, hi)
        out[x + offset, 0:4] = lo
        out[x + offset, 4:20] = v
        out[x + offset, 20:24] = hi


def solve(mu):
    g = lambda i: mu[i] - mu[i + 1]
    g00, g01, g02, g12, g22 = g(0), g(1), g(2), g(3), g(4)
    g11 = g02
    inverse = lambda d, scale: jnp.where(d > PIVOT * scale, 1.0 / d, 0.0)
    i0 = inverse(g00, 0.0 * g00)
    l10, l20 = g01 * i0, g02 * i0
    i1 = inverse(g11 - l10 * g01, g11)
    e = g12 - l10 * g02
    l21 = e * i1
    i2 = inverse(g22 - l20 * g02 - l21 * e, g22)
    c0 = mu[0]
    c1 = mu[1] - l10 * c0
    c2 = mu[2] - l20 * c0 - l21 * c1
    y2 = c2 * i2
    y1 = c1 * i1 - l21 * y2
    y0 = c0 * i0 - l10 * y1 - l20 * y2
    return y0, y1, y2


def coefficients(rows):
    total = jnp.sum(rows[...], axis=0, keepdims=True)
    at = lambda k: jnp.broadcast_to(total[:, k : k + 1], (1, 128))
    y = solve([at(k) for k in range(6)])
    c = (1.0, *y)
    mu = []
    for k in range(6):
        m = 0.0
        for i, (a, b) in enumerate(PAIRS):
            w = c[a] * c[b] * (1.0 if a == b else 2.0)
            m = m + w * at(6 + 10 * k + i)
        mu.append(m)
    v = solve(mu)
    scalar = lambda x: x[0, 0]
    return [scalar(x) for x in y], [[scalar(x * c[g]) for g in range(GENS)] for x in v]


def around(v, x, cx, cy, cz):
    c = v[x]
    y, z = cy[x], cz[x]
    return (
        cx[x] * v[x + 1]
        + cx[x - 1] * v[x - 1]
        + y * up_y(c)
        + dn_y(y * c)
        + z * up_z(c)
        + dn_z(z * c)
    )


def pressure_chain(start, p, cx, cy, cz, inv, t, n, part):
    def first(x):
        r = start(x) + around(p, x, cx, cy, cz)
        return [(n, (0, x), r), (t, (0, x), inv[x] * r)]

    loop(1, XE - 1, first, PW)
    for i in (1, 2):

        def follow(x):
            r = around(t.at[i - 1], x, cx, cy, cz)
            return [(n, (i, x), r), (t, (i, x), inv[x] * r)]

        loop(1 + i, XE - 1 - i, follow, PW)

    def final(x):
        return [(n, (3, x), around(t.at[2], x, cx, cy, cz))]

    loop(LOW, LOW + NX, final, PW)

    def body(x, acc):
        s = [t[i, LOW + x, 8:24] for i in range(3)]
        q = [n[i, LOW + x, 8:24] for i in range(4)]
        return tuple(v + s[i] * q[j] for v, (i, j) in zip(acc, LEVELS))

    sums = lax.fori_loop(0, NX, body, (jnp.zeros((NY, NZ), F32),) * 6)
    at = lax.broadcasted_iota(jnp.int32, (8, 128), 1)
    row = jnp.zeros((8, 128), F32)
    for k, v in enumerate(sums):
        row = jnp.where(at == k, jnp.sum(v), row)
    part[...] = row


def pressure_first_kernel(
    flags, mats, ids, p, f, low, high, yl, yh,
    code, pe, coef, t, part,
    fe, perm, stor, stab, n,
):
    cx, cy, cz, inv, diag, base, biot = (coef.at[i] for i in range(7))
    fill(code, XE, LOW, ids, low, high, (0, 0), yl, yh, 0, flags)
    fill(pe, XE, LOW, p, low, high, (7, 6), yl, yh, 21, flags)
    fill(fe.at[1:20], XE - 2, LOW - 1, f, low, high, (14, 12), yl, yh, 42, None)

    def tables(x):
        l, s, k, st, bi = lookup(code[x], mats, range(5))
        bi = 0.25 * bi
        st2 = bi * bi / jnp.maximum(l + (2.0 / 3.0) * s, 1e-30)
        return [(perm, x, k), (stor, x, st), (biot, x, bi), (stab, x, st2)]

    loop(0, XE, tables)

    def faces(x):
        k = perm[x]

        def harmonic(other):
            return (2.0 * DT) * k * other / jnp.maximum(k + other, 1e-30)

        return [
            (cx, x, harmonic(perm[x + 1])),
            (cy, x, harmonic(up_y(k))),
            (cz, x, harmonic(up_z(k))),
        ]

    loop(0, XE - 1, faces, 2)

    def diagonal(x):
        y, z = cy[x], cz[x]
        flow = cx[x] + cx[x - 1] + y + dn_y(y) + z + dn_z(z)
        inside = code[x] > 0.5
        d = stor[x] + stab[x] + flow
        return [
            (inv, x, jnp.where(inside, 1.0 / jnp.where(inside, d, 1.0), 0.0)),
            (diag, x, stab[x] - d),
            (base, x, stor[x] * pe[x] + DT * fe[x]),
        ]

    loop(1, XE - 1, diagonal, 2)
    pressure_chain(lambda x: base[x] + diag[x] * pe[x], pe, cx, cy, cz, inv, t, n, part)


def pressure_next_kernel(
    flags, coef, p, du, uo, low, high, yl, yh,
    pe, ue, t, part,
    de, n,
):
    cx, cy, cz, inv, diag, base, biot = (coef.at[i] for i in range(7))
    edge = lambda x, n: flags[0] if x < n else flags[1]
    zero = jnp.zeros((2, NZ), F32)
    for a in range(3):
        for x in range(20):
            k = 6 * (20 * a + x)
            out = de.at[a, x + 1]
            lo, hi = yl[k : k + 6] * flags[2], yh[k : k + 6] * flags[3]
            if 5 <= x < 15:
                out[4:28] = du[a, x - 5]
            else:
                outer = edge(x, 5)
                lo, hi = lo * outer, hi * outer
                ref = low.at[5 * a + x] if x < 5 else high.at[5 * a + x - 15]
                out[8:24] = ref[...] * outer
            if not 6 <= x < 14:
                lo, hi = lo * edge(x, 6), hi * edge(x, 6)
            out[0:2] = zero
            out[2:8] = lo
            out[24:30] = hi
            out[30:32] = zero
    for x in range(XE):
        k = 360 + 8 * x
        lo, hi = yl[k : k + 8] * flags[2], yh[k : k + 8] * flags[3]
        if not LOW <= x < LOW + NX:
            lo, hi = lo * edge(x, LOW), hi * edge(x, LOW)
        if 3 <= x < 18:
            pe[x, 8:24] = p[x - 3, 8:24]
        else:
            ref = low.at[15 + x] if x < 3 else high.at[15 + x - 18]
            pe[x, 8:24] = ref[...] * edge(x, LOW)
        pe[x, 0:8] = lo
        pe[x, 24:32] = hi

    def start(x):
        c2 = de[2, x]
        div = (
            de[0, x + 1] - de[0, x]
            + up_y(de[1, x]) - de[1, x]
            + up_z(c2) - c2
        )
        return base[x] - biot[x] * div + diag[x] * pe[x]

    pressure_chain(start, pe, cx, cy, cz, inv, t, n, part)
    for a in range(3):
        for m in range(ME):
            ue[a, m] = uo[a, m] + de[a, m + MO, 4:28]


def mech_chain(u, bf, pe, t, biot, mc, kept, q, load, carry, acc, s, part_p, part):
    sx, sy, sz, diag, lame, h0, h1, h2, kk = (mc.at[i] for i in range(9))
    h = (h0, h1, h2)

    def loads(m):
        x = m + MO
        bi = biot[x, 4:28]
        fields = [pe[x, 4:28]] + [t[i, x, 4:28] for i in range(3)]
        return [(load, (g, m), bi * v) for g, v in enumerate(fields)]

    loop(0, ME - 1, loads, 2)

    def ups(w, m):
        return (w[0, m + 1], up_y(w[1, m]), up_z(w[2, m]))

    def precondition(r, m):
        hs = [h[a][m] for a in range(3)]
        scaled = [r[a] * hs[a] for a in range(3)]
        k = kk[m] * (scaled[0] + scaled[1] + scaled[2])
        return [scaled[a] - hs[a] * k for a in range(3)]

    def pull(m):
        p = ups(u, m)
        return lame[m] * (p[0] + p[1] + p[2] - (u[0, m] + u[1, m] + u[2, m]))

    carry[0] = load[0, 0] - pull(0)

    def own(m):
        return jnp.where((m >= ML) & (m < ML + NX), m - ML, NX)

    def near(m):
        return jnp.where((m >= ML - 1) & (m <= ML + NX), m - ML + 1, NX + 2)

    def residual(m):
        for g in range(GENS):
            if g == 0:
                c = load[0, m] - pull(m)
                below = carry[0]
                d = diag[m]
                r = [
                    bf[a, m] - d * u[a, m] + around(u.at[a], m, sx, sy, sz) for a in range(3)
                ]
            else:
                c = load[g, m]
                below = load[g, m - 1]
                r = [0.0, 0.0, 0.0]
            low = (below, dn_y(c), dn_z(c))
            r = [r[a] + (low[a] - c) for a in range(3)]
            if g == 0:
                yield carry, 0, c
            z = precondition(r, m)
            for a in range(3):
                yield q, (0, g, a, own(m)), r[a]
                yield s, (0, g, a, m), z[a]
                yield kept, (g * 3 + a, near(m)), z[a]

    loop(1, ME - 1, residual)

    def basis(i, g):
        if i < 2:
            return s.at[i, g], 0
        k = (i * GENS + g) * 3
        return kept.at[k : k + 3], ML - 1

    def parts(w, m, o):
        c = [w[a, m - o] for a in range(3)]
        p = (w[0, m + 1 - o], up_y(c[1]), up_z(c[2]))
        total = p[0] + p[1] + p[2]
        l = lame[m]
        e = (c[0] + c[1] + c[2]) - total
        x, y, z = sx[m], sy[m], sz[m]
        above = x * c[0] + l * (p[0] + e)
        r = [
            x * p[0],
            y * p[1] + dn_y(y * c[1] + l * (p[1] + e)),
            z * p[2] + dn_z(z * c[2] + l * (p[2] + e)),
        ]
        return c, r, l * total, above

    for i in (1, 2, 3):
        for g in range(GENS):
            w, o = basis(i - 1, g)
            carry[g] = parts(w, i, o)[3]

        def follow(m):
            for g in range(GENS):
                w, o = basis(i - 1, g)
                c, r, push, above = parts(w, m, o)
                below = carry[g]
                yield carry, g, above
                x, xb, y, z = sx[m], sx[m - 1], sy[m], sz[m]
                r[0] = r[0] + push + below + (y * up_y(c[0]) + dn_y(y * c[0])) + (
                    z * up_z(c[0]) + dn_z(z * c[0])
                )
                r[1] = r[1] + push + (x * w[1, m + 1 - o] + xb * w[1, m - 1 - o]) + (
                    z * up_z(c[1]) + dn_z(z * c[1])
                )
                r[2] = r[2] + push + (x * w[2, m + 1 - o] + xb * w[2, m - 1 - o]) + (
                    y * up_y(c[2]) + dn_y(y * c[2])
                )
                slot = own(m) if i < 3 else m - ML
                for a in range(3):
                    yield q, (i, g, a, slot), r[a]
                if i < 3:
                    v = precondition(r, m)
                    for a in range(3):
                        if i == 1:
                            yield s, (i, g, a, m), v[a]
                        yield kept, ((i * GENS + g) * 3 + a, near(m)), v[a]

        loop(1 + i, ME - 1 - i, follow)

    top = lax.broadcasted_iota(jnp.int32, (8, NZ), 0) >= 4
    for k, (i, j) in enumerate(LEVELS):

        def body(x, sums):
            sums = list(sums)
            for a in range(3):
                v = [kept[(i * GENS + g) * 3 + a, 1 + x] for g in range(GENS)]
                w = [q[j, g, a, x] for g in range(GENS)]
                for pick_rows in (
                    lambda f: f[8:16],
                    lambda f: jnp.where(top, f[0:8], f[16:24]),
                ):
                    vt, wt = [pick_rows(f) for f in v], [pick_rows(f) for f in w]
                    sums = [c + vt[g] * wt[o] for c, (g, o) in zip(sums, PAIRS)]
            return tuple(sums)

        sums = lax.fori_loop(0, NX, body, (jnp.zeros((8, NZ), F32),) * len(PAIRS))
        for n, v in enumerate(sums):
            acc[10 * k + n] = v
    at = lax.broadcasted_iota(jnp.int32, (8, 128), 1)
    row = part_p[...]
    for k in range(60):
        row = jnp.where(at == k + 6, jnp.sum(acc[k]), row)
    for i in range(0, 128, 8):
        part[i : i + 8] = row


def mech_first_kernel(
    flags, mats, part_p, code, pe, coef, t, u, b, low, high, yl, yh,
    ue, be, mc, kept, part,
    q, load, shear, carry, acc, s,
):
    sx, sy, sz, diag, lame, h0, h1, h2, kk = (mc.at[i] for i in range(9))
    for a in range(3):
        fill_mech(ue.at[a], 16, 4, u.at[a], low, high, (4 * a, 4 * a), yl, yh, 8 * a, flags, 0)
        fill_mech(be.at[a], 14, 3, b.at[a], low, high, (12 + 3 * a, 12 + 3 * a), yl, yh, 24 + 7 * a, None, 1)

    def tables(m):
        l, g = lookup(code[m + MO, 4:28], mats, (0, 1))
        return [(lame, m, l), (shear, m, g)]

    loop(0, ME, tables)

    def faces(m):
        g = shear[m]
        return [
            (sx, m, 0.5 * (g + shear[m + 1])),
            (sy, m, 0.5 * (g + up_y(g))),
            (sz, m, 0.5 * (g + up_z(g))),
        ]

    loop(0, ME - 1, faces, 2)

    def diagonal(m):
        g, l = shear[m], lame[m]
        near = (
            shear[m + 1] + shear[m - 1] + up_y(g) + dn_y(g)
            + up_z(g) + dn_z(g)
        )
        d = 3.0 * g + 0.5 * near
        inside = g > 0.0
        lows = (lame[m - 1], dn_y(l), dn_z(l))
        hs = [jnp.where(inside, 1.0 / jnp.where(inside, d + v, 1.0), 0.0) for v in lows]
        k = l / (1.0 + l * (hs[0] + hs[1] + hs[2]))
        return [(diag, m, d), (h0, m, hs[0]), (h1, m, hs[1]), (h2, m, hs[2]), (kk, m, k)]

    loop(1, ME - 1, diagonal, 2)
    mech_chain(ue, be, pe, t, coef.at[6], mc, kept, q, load, carry, acc, s, part_p, part)


def mech_next_kernel(
    part_p, pe, coef, t, ue, be, mc,
    kept, part,
    q, load, carry, acc, s,
):
    mech_chain(ue, be, pe, t, coef.at[6], mc, kept, q, load, carry, acc, s, part_p, part)


def combine(v, kept, a, x):
    total = 0.0
    for i in range(3):
        for g in range(GENS):
            total = total + v[i][g] * kept[(i * GENS + g) * 3 + a, x]
    return total


def change_kernel(rows, t, pe, kept, u, du, pnew, unew, up, dn):
    y, v = coefficients(rows)
    for k in range(PK):
        x = k + MO
        w = pe[x] + (y[0] * t[0, x] + y[1] * t[1, x] + y[2] * t[2, x])
        pnew[k] = w
        i = k - ML
        if 1 <= i <= 3:
            up[14 + i] = w[8:24]
        if 3 <= i <= 5:
            dn[12 + i] = w[8:24]
    for a in range(3):
        for k in range(NX + 2):
            d = combine(v, kept, a, k)
            du[a, k] = d
            i = k - 1
            if 0 <= i < NX:
                unew[a, i] = u[a, i] + d[4:20]
            if 2 <= i <= 6:
                up[5 * a + i - 2] = d[4:20]
            if 1 <= i <= 5:
                dn[5 * a + i - 1] = d[4:20]


def pack_change_kernel(du, p, low, high, up, dn):
    for a in range(3):
        for x in range(20):
            if x < 5:
                ref, r = low.at[5 * a + x], 0
            elif x < 15:
                ref, r = du.at[a, x - 5], 4
            else:
                ref, r = high.at[5 * a + x - 15], 0
            k = 6 * (20 * a + x)
            up[k : k + 6] = ref[r + 10 : r + 16]
            dn[k : k + 6] = ref[r : r + 6]
    for x in range(XE):
        if x < 3:
            ref, r = low.at[15 + x], 0
        elif x < 18:
            ref, r = p.at[x - 3], 8
        else:
            ref, r = high.at[15 + x - 18], 0
        k = 360 + 8 * x
        up[k : k + 8] = ref[r + 8 : r + 16]
        dn[k : k + 8] = ref[r : r + 8]


def finish_kernel(rows, t, p, kept, u, unew, pnew):
    y, v = coefficients(rows)
    for x in range(NX):
        k = x + LOW
        w = p[k, 8:24] + (y[0] * t[0, k, 8:24] + y[1] * t[1, k, 8:24] + y[2] * t[2, k, 8:24])
        pnew[x] = w
        for a in range(3):
            unew[a, x] = u[a, x] + combine(v, kept, a, x + 1)[4:20]


def call(kernel, name, ins, outs, scratch=(), specs=None, cost=0, limit=12):
    return pl.pallas_call(
        kernel,
        name=name,
        out_shape=[jax.ShapeDtypeStruct(o, F32) for o in outs],
        in_specs=specs or [VM] * len(ins),
        out_specs=[VM] * len(outs),
        scratch_shapes=[pltpu.VMEM(s, F32) if isinstance(s, tuple) else s for s in scratch],
        compiler_params=pltpu.CompilerParams(vmem_limit_bytes=limit * 2**20),
        cost_estimate=pl.CostEstimate(flops=cost, bytes_accessed=0, transcendentals=0) if cost else None,
    )(*ins)


def neighbours(axis, size, up, dn):
    ring = [(i, (i + 1) % size) for i in range(size)]
    return lax.ppermute(up, axis, ring), lax.ppermute(dn, axis, [(b, a) for a, b in ring])


def gather_rows(part):
    return lax.all_to_all(part, ("gx", "gy"), 0, 0, tiled=True)


def on_device(gx_size, gy_size, u, p, b, f, ids, mats):
    gx, gy = lax.axis_index("gx"), lax.axis_index("gy")
    flags = jnp.stack([gx > 0, gx < gx_size - 1, gy > 0, gy < gy_size - 1]).astype(F32)
    wide, mech = (YE, NZ), (YM, NZ)
    up_p, dn_p, up_m, dn_m, own_code, own_p, own_f = call(
        pack_x_kernel,
        "pack_x",
        [pltpu.with_memory_space_constraint(v, pltpu.HBM) for v in (ids, p, f, u, b)],
        [(20, NY, NZ), (17, NY, NZ), (21, NY, NZ), (21, NY, NZ)] + [(NX, NY, NZ)] * 3,
        [pltpu.VMEM((NX, NY, NZ), jnp.int32), pltpu.SemaphoreType.DMA((19,))],
        [HB] * 5,
    )
    low_p, high_p = neighbours("gx", gx_size, up_p, dn_p)
    low_m, high_m = neighbours("gx", gx_size, up_m, dn_m)
    up, dn = call(
        pack_y_pressure_kernel, "pack_yp", (own_code, own_p, own_f, low_p, high_p), [(61, 8, NZ), (61, 8, NZ)], limit=4
    )
    yl_p, yh_p = neighbours("gy", gy_size, up, dn)
    up, dn = call(pack_y_mech_kernel, "pack_ym", (u, b, low_m, high_m), [(45, 8, NZ), (45, 8, NZ)], limit=4)
    yl_m, yh_m = neighbours("gy", gy_size, up, dn)
    code, pe, coef, t, part_p = call(
        pressure_first_kernel,
        "pressure_first",
        (flags, mats, own_code, own_p, own_f, low_p, high_p, yl_p, yh_p),
        [(XE, *wide), (XE, *wide), (7, XE, *wide), (3, XE, *wide), (8, 128)],
        [(XE, *wide)] * 4 + [(4, XE, *wide)],
        [SM, SM] + [VM] * 7,
        COST,
    )
    mech_scratch = [
        (4, GENS, 3, NX + 1, *mech),
        (GENS, ME, *mech),
        (GENS, *mech),
        (60, 8, NZ),
        (2, GENS, 3, ME, *mech),
    ]
    basis = (9 * GENS, NX + 3, *mech)
    ue, be, mc, s, part = call(
        mech_first_kernel,
        "mech_first",
        (flags, mats, part_p, code, pe, coef, t, u, b, low_m, high_m, yl_m, yh_m),
        [(3, ME, *mech), (3, ME, *mech), (9, ME, *mech), basis, (128, 128)],
        mech_scratch[:2] + [(ME, *mech)] + mech_scratch[2:],
        [SM, SM] + [VM] * 11,
        COST,
        24,
    )
    rows = gather_rows(part)
    du, p1, u1, up, dn = call(
        change_kernel,
        "change",
        (rows, t, pe, s, u),
        [(3, NX + 2, *mech), (PK, *wide), (3, NX, NY, NZ), (18, NY, NZ), (18, NY, NZ)],
    )
    low, high = neighbours("gx", gx_size, up, dn)
    up, dn = call(pack_change_kernel, "pack_change", (du, p1, low, high), [(528, NZ), (528, NZ)])
    yl, yh = neighbours("gy", gy_size, up, dn)
    pe, ue, t, part_p = call(
        pressure_next_kernel,
        "pressure_next",
        (flags, coef, p1, du, ue, low, high, yl, yh),
        [(XE, *wide), (3, ME, *mech), (3, XE, *wide), (8, 128)],
        [(3, XE, *wide), (4, XE, *wide)],
        [SM] + [VM] * 8,
        COST,
    )
    s, part = call(
        mech_next_kernel,
        "mech_next",
        (part_p, pe, coef, t, ue, be, mc),
        [basis, (128, 128)],
        mech_scratch,
        None,
        COST,
        24,
    )
    rows = gather_rows(part)
    u2, p2 = call(
        finish_kernel,
        "finish",
        (rows, t, pe, s, u1),
        [(3, NX, NY, NZ), (NX, NY, NZ)],
    )
    return u2, p2


def solution(mesh):
    body = functools.partial(on_device, mesh.shape["gx"], mesh.shape["gy"])
    field, vector = P("gx", "gy", None), P(None, "gx", "gy", None)
    return jax.shard_map(
        body,
        mesh=mesh,
        in_specs=(vector, field, vector, field, field, P()),
        out_specs=(vector, field),
        check_vma=False,
    )
```

```python
import functools

import jax
import jax.numpy as jnp
from jax import lax
from jax.experimental import pallas as pl
from jax.experimental.pallas import tpu as pltpu
from jax.sharding import PartitionSpec as P

F32 = jnp.float32
DT = 4.0
NX, NY, NZ = 8, 16, 256
YE = 32
YM = 24
GENS = 4
PAIRS = [(a, b) for a in range(GENS) for b in range(a, GENS)]
LEVELS = ((0, 0), (0, 1), (1, 1), (1, 2), (2, 2), (2, 3))
LOW, HIGH = 6, 6
XE = LOW + NX + HIGH
ML, MH = 3, 4
ME = ML + NX + MH
MO = LOW - ML
PK = 3 + NX + 3
PIVOT = 2e-7
PW = 4
COST = 200_000_000

VM = pl.BlockSpec(memory_space=pltpu.VMEM)
SM = pl.BlockSpec(memory_space=pltpu.SMEM)
HB = pl.BlockSpec(memory_space=pltpu.HBM)


def up_y(v):
    n = v.shape[0] // 8
    turned = [pltpu.roll(v[8 * k : 8 * k + 8], 7, 0) for k in range(n)]
    inner = lax.broadcasted_iota(jnp.int32, turned[0].shape, 0) < 7
    joined = [jnp.where(inner, turned[k], turned[k + 1]) for k in range(n - 1)]
    return jnp.concatenate([*joined, turned[n - 1]], axis=0)


def dn_y(v):
    n = v.shape[0] // 8
    turned = [pltpu.roll(v[8 * k : 8 * k + 8], 1, 0) for k in range(n)]
    inner = lax.broadcasted_iota(jnp.int32, turned[0].shape, 0) > 0
    joined = [jnp.where(inner, turned[k], turned[k - 1]) for k in range(1, n)]
    return jnp.concatenate([turned[0], *joined], axis=0)


def up_z(v):
    low, high = pltpu.roll(v[:, :128], 127, 1), pltpu.roll(v[:, 128:], 127, 1)
    inner = lax.broadcasted_iota(jnp.int32, low.shape, 1) < 127
    return jnp.concatenate([jnp.where(inner, low, high), jnp.where(inner, high, 0.0)], axis=1)


def dn_z(v):
    low, high = pltpu.roll(v[:, :128], 1, 1), pltpu.roll(v[:, 128:], 1, 1)
    inner = lax.broadcasted_iota(jnp.int32, low.shape, 1) > 0
    return jnp.concatenate([jnp.where(inner, low, 0.0), jnp.where(inner, high, low)], axis=1)


def loop(low, high, compute, width=1):
    def group(x, count):
        for i in range(count):
            for ref, index, value in compute(x + i):
                ref[index] = value

    steps = (high - low) // width

    def step(k, carry):
        group(low + k * width, width)
        return carry

    lax.fori_loop(0, steps, step, 0)
    if (high - low) % width:
        group(low + steps * width, (high - low) % width)


def lookup(code, mats, rows):
    found = [jnp.zeros(code.shape, F32) for _ in rows]
    for m in range(8):
        hit = code == float(m + 1)
        found = [jnp.where(hit, mats[r, m], v) for r, v in zip(rows, found)]
    return found


def pack_x_kernel(ids, p, f, u, b, up_p, dn_p, up_m, dn_m, code, pv, fv, raw, sems):
    copies = []

    def take(src, dst):
        copies.append(pltpu.make_async_copy(src, dst, sems.at[len(copies)]))
        copies[-1].start()

    take(ids, raw)
    take(p, pv)
    take(f, fv)
    take(p.at[2:8], up_p.at[6:12])
    take(p.at[0:6], dn_p.at[6:12])
    take(f.at[3:8], up_p.at[12:17])
    take(f.at[0:5], dn_p.at[12:17])
    for a in range(3):
        take(u.at[a, 5:8], up_m.at[3 * a : 3 * a + 3])
        take(u.at[a, 0:4], dn_m.at[4 * a : 4 * a + 4])
        take(b.at[a, 6:8], up_m.at[9 + 2 * a : 11 + 2 * a])
        take(b.at[a, 0:3], dn_m.at[12 + 3 * a : 15 + 3 * a])
    copies[0].wait()
    for x in range(NX):
        c = (raw[x] + 1).astype(F32)
        code[x] = c
        if x >= 2:
            up_p[x - 2] = c
        if x < 6:
            dn_p[x] = c
    for copy in copies[1:]:
        copy.wait()


def pick(x, low, own, high, first, n_low):
    if x < n_low:
        return low, first[0] + x
    if x < n_low + NX:
        return own, x - n_low
    return high, first[1] + x - n_low - NX


def pack_y_pressure_kernel(ids, p, f, low, high, up, dn):
    for x in range(XE):
        ref, i = pick(x, low, ids, high, (0, 0), LOW)
        up[x] = ref[i, 8:16]
        dn[x] = ref[i, 0:8]
        ref, i = pick(x, low, p, high, (6, 6), LOW)
        up[20 + x] = ref[i, 8:16]
        dn[20 + x] = ref[i, 0:8]
    for x in range(XE - 2):
        ref, i = pick(x, low, f, high, (12, 12), LOW - 1)
        up[40 + x] = ref[i, 8:16]
        dn[40 + x] = ref[i, 0:8]


def pack_y_mech_kernel(u, b, low, high, up, dn):
    for a in range(3):
        for m in range(ME):
            ref, i = pick(m, low, u.at[a], high, (3 * a, 4 * a), ML)
            k, r = 8 * a + m // 2, 4 * (m % 2)
            up[k, r : r + 4] = ref[i, 12:16]
            dn[k, r : r + 4] = ref[i, 0:4]
        for m in range(ME - 2):
            ref, i = pick(m, low, b.at[a], high, (9 + 2 * a, 12 + 3 * a), ML - 1)
            k, r = 24 + 7 * a + m // 2, 4 * (m % 2)
            up[k, r : r + 4] = ref[i, 12:16]
            dn[k, r : r + 4] = ref[i, 0:4]


def masked(x, n_low, flags, v, lo, hi):
    if flags is None:
        return v, lo, hi
    lo, hi = (lo * flags[2], hi * flags[3])
    if n_low <= x < n_low + NX:
        return v, lo, hi
    edge = flags[0] if x < n_low else flags[1]
    return v * edge, lo * edge, hi * edge


def fill(out, n, n_low, own, low, high, first, yl, yh, k, flags):
    for x in range(n):
        ref, i = pick(x, low, own, high, first, n_low)
        v, lo, hi = masked(x, n_low, flags, ref[i], yl[k + x], yh[k + x])
        out[x, 8:24] = v
        out[x, 0:8] = lo
        out[x, 24:32] = hi


def fill_mech(out, n, n_low, own, low, high, first, yl, yh, k, flags, offset):
    for x in range(n):
        ref, i = pick(x, low, own, high, first, n_low)
        r = 4 * (x % 2)
        lo, hi = yl[k + x // 2, r : r + 4], yh[k + x // 2, r : r + 4]
        v, lo, hi = masked(x, n_low, flags, ref[i], lo, hi)
        out[x + offset, 0:4] = lo
        out[x + offset, 4:20] = v
        out[x + offset, 20:24] = hi


def solve(mu):
    g = lambda i: mu[i] - mu[i + 1]
    g00, g01, g02, g12, g22 = g(0), g(1), g(2), g(3), g(4)
    g11 = g02
    inverse = lambda d, scale: jnp.where(d > PIVOT * scale, 1.0 / d, 0.0)
    i0 = inverse(g00, 0.0 * g00)
    l10, l20 = g01 * i0, g02 * i0
    i1 = inverse(g11 - l10 * g01, g11)
    e = g12 - l10 * g02
    l21 = e * i1
    i2 = inverse(g22 - l20 * g02 - l21 * e, g22)
    c0 = mu[0]
    c1 = mu[1] - l10 * c0
    c2 = mu[2] - l20 * c0 - l21 * c1
    y2 = c2 * i2
    y1 = c1 * i1 - l21 * y2
    y0 = c0 * i0 - l10 * y1 - l20 * y2
    return y0, y1, y2


def coefficients(rows):
    total = jnp.sum(rows[...], axis=0, keepdims=True)
    at = lambda k: jnp.broadcast_to(total[:, k : k + 1], (1, 128))
    y = solve([at(k) for k in range(6)])
    c = (1.0, *y)
    mu = []
    for k in range(6):
        m = 0.0
        for i, (a, b) in enumerate(PAIRS):
            w = c[a] * c[b] * (1.0 if a == b else 2.0)
            m = m + w * at(6 + 10 * k + i)
        mu.append(m)
    v = solve(mu)
    scalar = lambda x: x[0, 0]
    return [scalar(x) for x in y], [[scalar(x * c[g]) for g in range(GENS)] for x in v]


def around(v, x, cx, cy, cz):
    c = v[x]
    y, z = cy[x], cz[x]
    return (
        cx[x] * v[x + 1]
        + cx[x - 1] * v[x - 1]
        + y * up_y(c)
        + dn_y(y * c)
        + z * up_z(c)
        + dn_z(z * c)
    )


def pressure_chain(start, p, cx, cy, cz, inv, t, n, part):
    def first(x):
        r = start(x) + around(p, x, cx, cy, cz)
        return [(n, (0, x), r), (t, (0, x), inv[x] * r)]

    loop(1, XE - 1, first, PW)
    for i in (1, 2):

        def follow(x):
            r = around(t.at[i - 1], x, cx, cy, cz)
            return [(n, (i, x), r), (t, (i, x), inv[x] * r)]

        loop(1 + i, XE - 1 - i, follow, PW)

    def final(x):
        v = t[2, x]
        e = cx[x] * t[2, x + 1] + cy[x] * up_y(v) + cz[x] * up_z(v)
        return [(n, (3, x), 2.0 * e)]

    loop(LOW, LOW + NX, final, PW)

    def body(x, acc):
        s = [t[i, LOW + x, 8:24] for i in range(3)]
        q = [n[i, LOW + x, 8:24] for i in range(4)]
        return tuple(v + s[i] * q[j] for v, (i, j) in zip(acc, LEVELS))

    sums = lax.fori_loop(0, NX, body, (jnp.zeros((NY, NZ), F32),) * 6)
    at = lax.broadcasted_iota(jnp.int32, (8, 128), 1)
    row = jnp.zeros((8, 128), F32)
    for k, v in enumerate(sums):
        row = jnp.where(at == k, jnp.sum(v), row)
    part[...] = row


def pressure_first_kernel(
    flags, mats, ids, p, f, low, high, yl, yh,
    code, pe, coef, t, part,
    fe, perm, stor, stab, n,
):
    cx, cy, cz, inv, diag, base, biot = (coef.at[i] for i in range(7))
    fill(code, XE, LOW, ids, low, high, (0, 0), yl, yh, 0, flags)
    fill(pe, XE, LOW, p, low, high, (6, 6), yl, yh, 20, flags)
    fill(fe.at[1 : XE - 1], XE - 2, LOW - 1, f, low, high, (12, 12), yl, yh, 40, None)

    def tables(x):
        l, s, k, st, bi = lookup(code[x], mats, range(5))
        bi = 0.25 * bi
        st2 = bi * bi / jnp.maximum(l + (2.0 / 3.0) * s, 1e-30)
        return [(perm, x, k), (stor, x, st), (biot, x, bi), (stab, x, st2)]

    loop(0, XE, tables)

    def faces(x):
        k = perm[x]

        def harmonic(other):
            return (2.0 * DT) * k * other / jnp.maximum(k + other, 1e-30)

        return [
            (cx, x, harmonic(perm[x + 1])),
            (cy, x, harmonic(up_y(k))),
            (cz, x, harmonic(up_z(k))),
        ]

    loop(0, XE - 1, faces, 2)

    def diagonal(x):
        y, z = cy[x], cz[x]
        flow = cx[x] + cx[x - 1] + y + dn_y(y) + z + dn_z(z)
        inside = code[x] > 0.5
        d = stor[x] + stab[x] + flow
        return [
            (inv, x, jnp.where(inside, 1.0 / jnp.where(inside, d, 1.0), 0.0)),
            (diag, x, stab[x] - d),
            (base, x, stor[x] * pe[x] + DT * fe[x]),
        ]

    loop(1, XE - 1, diagonal, 2)
    pressure_chain(lambda x: base[x] + diag[x] * pe[x], pe, cx, cy, cz, inv, t, n, part)


def pressure_next_kernel(
    flags, coef, p, du, uo, low, high, yl, yh,
    pe, ue, t, part,
    de, n,
):
    cx, cy, cz, inv, diag, base, biot = (coef.at[i] for i in range(7))
    edge = lambda x, n: flags[0] if x < n else flags[1]
    zero = jnp.zeros((2, NZ), F32)
    for a in range(3):
        for x in range(19):
            k = 6 * (19 * a + x)
            out = de.at[a, x + 1]
            lo, hi = yl[k : k + 6] * flags[2], yh[k : k + 6] * flags[3]
            if 5 <= x < 14:
                out[4:28] = du[a, x - 5]
            else:
                outer = edge(x, 5)
                lo, hi = lo * outer, hi * outer
                ref = low.at[5 * a + x] if x < 5 else high.at[5 * a + x - 14]
                out[8:24] = ref[...] * outer
            if x == 13:
                lo, hi = lo * flags[1], hi * flags[1]
            out[0:2] = zero
            out[2:8] = lo
            out[24:30] = hi
            out[30:32] = zero
    for x in range(XE):
        k = 344 + 8 * x
        lo, hi = yl[k : k + 8] * flags[2], yh[k : k + 8] * flags[3]
        if not LOW <= x < LOW + NX:
            lo, hi = lo * edge(x, LOW), hi * edge(x, LOW)
        if 3 <= x < 17:
            pe[x, 8:24] = p[x - 3, 8:24]
        else:
            ref = low.at[15 + x] if x < 3 else high.at[15 + x - 17]
            pe[x, 8:24] = ref[...] * edge(x, LOW)
        pe[x, 0:8] = lo
        pe[x, 24:32] = hi

    def start(x):
        c2 = de[2, x]
        div = (
            de[0, x + 1] - de[0, x]
            + up_y(de[1, x]) - de[1, x]
            + up_z(c2) - c2
        )
        return base[x] - biot[x] * div + diag[x] * pe[x]

    pressure_chain(start, pe, cx, cy, cz, inv, t, n, part)
    for a in range(3):
        for m in range(ME):
            ue[a, m] = uo[a, m] + de[a, m + MO, 4:28]


def mech_chain(u, bf, pe, t, biot, mc, kept, q, load, carry, acc, s, tg, part_p, part):
    sx, sy, sz, diag, lame, h0, h1, h2, kk = (mc.at[i] for i in range(9))
    h = (h0, h1, h2)

    def loads(m):
        x = m + MO
        bi = biot[x, 4:28]
        fields = [pe[x, 4:28]] + [t[i, x, 4:28] for i in range(3)]
        return [(load, (g, m), bi * v) for g, v in enumerate(fields)]

    loop(0, ME - 1, loads, 2)

    def ups(w, m):
        return (w[0, m + 1], up_y(w[1, m]), up_z(w[2, m]))

    def precondition(r, m):
        hs = [h[a][m] for a in range(3)]
        scaled = [r[a] * hs[a] for a in range(3)]
        k = kk[m] * (scaled[0] + scaled[1] + scaled[2])
        return [scaled[a] - hs[a] * k for a in range(3)]

    def pull(m):
        p = ups(u, m)
        return lame[m] * (p[0] + p[1] + p[2] - (u[0, m] + u[1, m] + u[2, m]))

    carry[0] = load[0, 0] - pull(0)

    def own(m):
        return jnp.where((m >= ML) & (m < ML + NX), m - ML, NX)

    def near(m):
        return jnp.where((m >= ML) & (m <= ML + NX), m - ML, NX + 1)

    def residual(m):
        for g in range(GENS):
            if g == 0:
                c = load[0, m] - pull(m)
                below = carry[0]
                d = diag[m]
                r = [
                    bf[a, m] - d * u[a, m] + around(u.at[a], m, sx, sy, sz) for a in range(3)
                ]
            else:
                c = load[g, m]
                below = load[g, m - 1]
                r = [0.0, 0.0, 0.0]
            low = (below, dn_y(c), dn_z(c))
            r = [r[a] + (low[a] - c) for a in range(3)]
            if g == 0:
                yield carry, 0, c
            z = precondition(r, m)
            for a in range(3):
                yield q, (0, g, a, own(m)), r[a]
                yield s, (0, g, a, m), z[a]
                yield kept, (g * 3 + a, near(m)), z[a]

    loop(1, ME - 1, residual, 2)

    def basis(i, g):
        if i < 2:
            return s.at[i, g], 0
        k = (i * GENS + g) * 3
        return kept.at[k : k + 3], ML

    def parts(w, m, o):
        c = [w[a, m - o] for a in range(3)]
        p = (w[0, m + 1 - o], up_y(c[1]), up_z(c[2]))
        total = p[0] + p[1] + p[2]
        l = lame[m]
        e = (c[0] + c[1] + c[2]) - total
        x, y, z = sx[m], sy[m], sz[m]
        above = x * c[0] + l * (p[0] + e)
        r = [
            x * p[0],
            y * p[1] + dn_y(y * c[1] + l * (p[1] + e)),
            z * p[2] + dn_z(z * c[2] + l * (p[2] + e)),
        ]
        return c, r, l * total, above

    for i in (1, 2):
        for g in range(GENS):
            w, o = basis(i - 1, g)
            carry[g] = parts(w, i, o)[3]

        def follow(m):
            for g in range(GENS):
                w, o = basis(i - 1, g)
                c, r, push, above = parts(w, m, o)
                below = carry[g]
                yield carry, g, above
                x, xb, y, z = sx[m], sx[m - 1], sy[m], sz[m]
                r[0] = r[0] + push + below + (y * up_y(c[0]) + dn_y(y * c[0])) + (
                    z * up_z(c[0]) + dn_z(z * c[0])
                )
                r[1] = r[1] + push + (x * w[1, m + 1 - o] + xb * w[1, m - 1 - o]) + (
                    z * up_z(c[1]) + dn_z(z * c[1])
                )
                r[2] = r[2] + push + (x * w[2, m + 1 - o] + xb * w[2, m - 1 - o]) + (
                    y * up_y(c[2]) + dn_y(y * c[2])
                )
                v = precondition(r, m)
                for a in range(3):
                    yield q, (i, g, a, own(m)), r[a]
                    if i == 1:
                        yield s, (i, g, a, m), v[a]
                    yield kept, ((i * GENS + g) * 3 + a, near(m)), v[a]

        loop(1 + i, ME - 1 - i, follow)

    def energy(m):
        l, x, y, z = lame[m], sx[m], sy[m], sz[m]
        half = (0.5 * lame[m - 1], 0.5 * dn_y(l), 0.5 * dn_z(l))
        for g in range(GENS):
            w, o = basis(2, g)
            total = 0.0
            for a in range(3):
                c = w[a, m - o]
                up = (w[a, m + 1 - o], up_y(c), up_z(c))
                total = total + up[a]
                yield q, (3, g, a, m - ML), x * up[0] + y * up[1] + z * up[2] + half[a] * c
            near_sum = w[0, m - o] + w[1, m - o] + w[2, m - o]
            yield tg, (0, g, m - ML), total
            yield tg, (1, g, m - ML), l * (near_sum - 0.5 * total)

    loop(ML, ML + NX, energy)

    top = lax.broadcasted_iota(jnp.int32, (8, NZ), 0) >= 4
    for k, (i, j) in enumerate(LEVELS):

        def body(step, sums):
            sums = list(sums)
            for x in (2 * step, 2 * step + 1):
                for a in range(3 if j < 3 else 4):
                    if a < 3:
                        v = [kept[(i * GENS + g) * 3 + a, x] for g in range(GENS)]
                        w = [q[j, g, a, x] for g in range(GENS)]
                    else:
                        v = [tg[0, g, x] for g in range(GENS)]
                        w = [tg[1, g, x] for g in range(GENS)]
                    for pick_rows in (
                        lambda f: f[8:16],
                        lambda f: jnp.where(top, f[0:8], f[16:24]),
                    ):
                        vt, wt = [pick_rows(f) for f in v], [pick_rows(f) for f in w]
                        sums = [c + vt[g] * wt[o] for c, (g, o) in zip(sums, PAIRS)]
                        if j == 3:
                            sums = [c + vt[o] * wt[g] for c, (g, o) in zip(sums, PAIRS)]
            return tuple(sums)

        sums = lax.fori_loop(0, NX // 2, body, (jnp.zeros((8, NZ), F32),) * len(PAIRS))
        for n, v in enumerate(sums):
            acc[10 * k + n] = v
    at = lax.broadcasted_iota(jnp.int32, (8, 128), 1)
    row = part_p[...]
    for k in range(60):
        row = jnp.where(at == k + 6, jnp.sum(acc[k]), row)
    for i in range(0, 128, 8):
        part[i : i + 8] = row


def mech_first_kernel(
    flags, mats, part_p, code, pe, coef, t, u, b, low, high, yl, yh,
    ue, be, mc, kept, part,
    q, load, shear, carry, acc, s, tg,
):
    sx, sy, sz, diag, lame, h0, h1, h2, kk = (mc.at[i] for i in range(9))
    for a in range(3):
        fill_mech(ue.at[a], ME, ML, u.at[a], low, high, (3 * a, 4 * a), yl, yh, 8 * a, flags, 0)
        fill_mech(
            be.at[a], ME - 2, ML - 1, b.at[a], low, high, (9 + 2 * a, 12 + 3 * a), yl, yh, 24 + 7 * a, None, 1
        )

    def tables(m):
        l, g = lookup(code[m + MO, 4:28], mats, (0, 1))
        return [(lame, m, l), (shear, m, g)]

    loop(0, ME, tables)

    def faces(m):
        g = shear[m]
        return [
            (sx, m, 0.5 * (g + shear[m + 1])),
            (sy, m, 0.5 * (g + up_y(g))),
            (sz, m, 0.5 * (g + up_z(g))),
        ]

    loop(0, ME - 1, faces, 2)

    def diagonal(m):
        g, l = shear[m], lame[m]
        near = (
            shear[m + 1] + shear[m - 1] + up_y(g) + dn_y(g)
            + up_z(g) + dn_z(g)
        )
        d = 3.0 * g + 0.5 * near
        inside = g > 0.0
        lows = (lame[m - 1], dn_y(l), dn_z(l))
        hs = [jnp.where(inside, 1.0 / jnp.where(inside, d + v, 1.0), 0.0) for v in lows]
        k = l / (1.0 + l * (hs[0] + hs[1] + hs[2]))
        return [(diag, m, d), (h0, m, hs[0]), (h1, m, hs[1]), (h2, m, hs[2]), (kk, m, k)]

    loop(1, ME - 1, diagonal, 2)
    mech_chain(ue, be, pe, t, coef.at[6], mc, kept, q, load, carry, acc, s, tg, part_p, part)


def mech_next_kernel(
    part_p, pe, coef, t, ue, be, mc,
    kept, part,
    q, load, carry, acc, s, tg,
):
    mech_chain(ue, be, pe, t, coef.at[6], mc, kept, q, load, carry, acc, s, tg, part_p, part)


def combine(v, kept, a, x):
    total = 0.0
    for i in range(3):
        for g in range(GENS):
            total = total + v[i][g] * kept[(i * GENS + g) * 3 + a, x]
    return total


def change_kernel(rows, t, pe, kept, u, du, pnew, unew, up, dn):
    y, v = coefficients(rows)
    for k in range(PK):
        x = k + MO
        w = pe[x] + (y[0] * t[0, x] + y[1] * t[1, x] + y[2] * t[2, x])
        pnew[k] = w
        i = k - ML
        if 2 <= i <= 4:
            up[13 + i] = w[8:24]
        if 3 <= i <= 5:
            dn[12 + i] = w[8:24]
    for a in range(3):
        for i in range(NX + 1):
            d = combine(v, kept, a, i)
            du[a, i] = d
            if i < NX:
                unew[a, i] = u[a, i] + d[4:20]
            if 3 <= i <= 7:
                up[5 * a + i - 3] = d[4:20]
            if 1 <= i <= 5:
                dn[5 * a + i - 1] = d[4:20]


def pack_change_kernel(du, p, low, high, up, dn):
    for a in range(3):
        for x in range(19):
            if x < 5:
                ref, r = low.at[5 * a + x], 0
            elif x < 14:
                ref, r = du.at[a, x - 5], 4
            else:
                ref, r = high.at[5 * a + x - 14], 0
            k = 6 * (19 * a + x)
            up[k : k + 6] = ref[r + 10 : r + 16]
            dn[k : k + 6] = ref[r : r + 6]
    for x in range(XE):
        if x < 3:
            ref, r = low.at[15 + x], 0
        elif x < 17:
            ref, r = p.at[x - 3], 8
        else:
            ref, r = high.at[15 + x - 17], 0
        k = 344 + 8 * x
        up[k : k + 8] = ref[r + 8 : r + 16]
        dn[k : k + 8] = ref[r : r + 8]


def finish_kernel(rows, t, p, kept, u, unew, pnew):
    y, v = coefficients(rows)
    for x in range(NX):
        k = x + LOW
        w = p[k, 8:24] + (y[0] * t[0, k, 8:24] + y[1] * t[1, k, 8:24] + y[2] * t[2, k, 8:24])
        pnew[x] = w
        for a in range(3):
            unew[a, x] = u[a, x] + combine(v, kept, a, x)[4:20]


def call(kernel, name, ins, outs, scratch=(), specs=None, cost=0, limit=12):
    return pl.pallas_call(
        kernel,
        name=name,
        out_shape=[jax.ShapeDtypeStruct(o, F32) for o in outs],
        in_specs=specs or [VM] * len(ins),
        out_specs=[VM] * len(outs),
        scratch_shapes=[pltpu.VMEM(s, F32) if isinstance(s, tuple) else s for s in scratch],
        compiler_params=pltpu.CompilerParams(vmem_limit_bytes=limit * 2**20),
        cost_estimate=pl.CostEstimate(flops=cost, bytes_accessed=0, transcendentals=0) if cost else None,
    )(*ins)


def neighbours(axis, size, up, dn):
    ring = [(i, (i + 1) % size) for i in range(size)]
    return lax.ppermute(up, axis, ring), lax.ppermute(dn, axis, [(b, a) for a, b in ring])


def gather_rows(part):
    return lax.all_to_all(part, ("gx", "gy"), 0, 0, tiled=True)


def on_device(gx_size, gy_size, u, p, b, f, ids, mats):
    gx, gy = lax.axis_index("gx"), lax.axis_index("gy")
    flags = jnp.stack([gx > 0, gx < gx_size - 1, gy > 0, gy < gy_size - 1]).astype(F32)
    wide, mech = (YE, NZ), (YM, NZ)
    up_p, dn_p, up_m, dn_m, own_code, own_p, own_f = call(
        pack_x_kernel,
        "pack_x",
        [pltpu.with_memory_space_constraint(v, pltpu.HBM) for v in (ids, p, f, u, b)],
        [(17, NY, NZ), (17, NY, NZ), (15, NY, NZ), (21, NY, NZ)] + [(NX, NY, NZ)] * 3,
        [pltpu.VMEM((NX, NY, NZ), jnp.int32), pltpu.SemaphoreType.DMA((19,))],
        [HB] * 5,
    )
    low_p, high_p = neighbours("gx", gx_size, up_p, dn_p)
    low_m, high_m = neighbours("gx", gx_size, up_m, dn_m)
    up, dn = call(
        pack_y_pressure_kernel, "pack_yp", (own_code, own_p, own_f, low_p, high_p), [(58, 8, NZ), (58, 8, NZ)], limit=4
    )
    yl_p, yh_p = neighbours("gy", gy_size, up, dn)
    up, dn = call(pack_y_mech_kernel, "pack_ym", (u, b, low_m, high_m), [(45, 8, NZ), (45, 8, NZ)], limit=4)
    yl_m, yh_m = neighbours("gy", gy_size, up, dn)
    code, pe, coef, t, part_p = call(
        pressure_first_kernel,
        "pressure_first",
        (flags, mats, own_code, own_p, own_f, low_p, high_p, yl_p, yh_p),
        [(XE, *wide), (XE, *wide), (7, XE, *wide), (3, XE, *wide), (8, 128)],
        [(XE, *wide)] * 4 + [(4, XE, *wide)],
        [SM, SM] + [VM] * 7,
        COST,
    )
    mech_scratch = [
        (4, GENS, 3, NX + 1, *mech),
        (GENS, ME, *mech),
        (GENS, *mech),
        (60, 8, NZ),
        (2, GENS, 3, ME, *mech),
        (2, GENS, NX, *mech),
    ]
    basis = (9 * GENS, NX + 2, *mech)
    ue, be, mc, s, part = call(
        mech_first_kernel,
        "mech_first",
        (flags, mats, part_p, code, pe, coef, t, u, b, low_m, high_m, yl_m, yh_m),
        [(3, ME, *mech), (3, ME, *mech), (9, ME, *mech), basis, (128, 128)],
        mech_scratch[:2] + [(ME, *mech)] + mech_scratch[2:],
        [SM, SM] + [VM] * 11,
        COST,
        26,
    )
    rows = gather_rows(part)
    du, p1, u1, up, dn = call(
        change_kernel,
        "change",
        (rows, t, pe, s, u),
        [(3, NX + 1, *mech), (PK, *wide), (3, NX, NY, NZ), (18, NY, NZ), (18, NY, NZ)],
    )
    low, high = neighbours("gx", gx_size, up, dn)
    up, dn = call(pack_change_kernel, "pack_change", (du, p1, low, high), [(504, NZ), (504, NZ)])
    yl, yh = neighbours("gy", gy_size, up, dn)
    pe, ue, t, part_p = call(
        pressure_next_kernel,
        "pressure_next",
        (flags, coef, p1, du, ue, low, high, yl, yh),
        [(XE, *wide), (3, ME, *mech), (3, XE, *wide), (8, 128)],
        [(3, XE, *wide), (4, XE, *wide)],
        [SM] + [VM] * 8,
        COST,
    )
    s, part = call(
        mech_next_kernel,
        "mech_next",
        (part_p, pe, coef, t, ue, be, mc),
        [basis, (128, 128)],
        mech_scratch,
        None,
        COST,
        26,
    )
    rows = gather_rows(part)
    u2, p2 = call(
        finish_kernel,
        "finish",
        (rows, t, pe, s, u1),
        [(3, NX, NY, NZ), (NX, NY, NZ)],
    )
    return u2, p2


def solution(mesh):
    body = functools.partial(on_device, mesh.shape["gx"], mesh.shape["gy"])
    field, vector = P("gx", "gy", None), P(None, "gx", "gy", None)
    return jax.shard_map(
        body,
        mesh=mesh,
        in_specs=(vector, field, vector, field, field, P()),
        out_specs=(vector, field),
        check_vma=False,
    )
```

```python
import functools

import jax
import jax.numpy as jnp
from jax import lax
from jax.experimental import pallas as pl
from jax.experimental.pallas import tpu as pltpu
from jax.sharding import PartitionSpec as P

F32 = jnp.float32
DT = 4.0
NX, NY, NZ = 8, 16, 256
YE = 32
YM = 24
GENS = 4
PAIRS = [(a, b) for a in range(GENS) for b in range(a, GENS)]
LEVELS = ((0, 0), (0, 1), (1, 1), (1, 2), (2, 2), (2, 3))
LOW, HIGH = 6, 6
XE = LOW + NX + HIGH
ML, MH = 3, 4
ME = ML + NX + MH
MO = LOW - ML
PK = 3 + NX + 3
PIVOT = 2e-7
PW = 4
COST = 200_000_000

VM = pl.BlockSpec(memory_space=pltpu.VMEM)
SM = pl.BlockSpec(memory_space=pltpu.SMEM)
HB = pl.BlockSpec(memory_space=pltpu.HBM)


def up_y(v):
    n = v.shape[0] // 8
    turned = [pltpu.roll(v[8 * k : 8 * k + 8], 7, 0) for k in range(n)]
    inner = lax.broadcasted_iota(jnp.int32, turned[0].shape, 0) < 7
    joined = [jnp.where(inner, turned[k], turned[k + 1]) for k in range(n - 1)]
    return jnp.concatenate([*joined, turned[n - 1]], axis=0)


def dn_y(v):
    n = v.shape[0] // 8
    turned = [pltpu.roll(v[8 * k : 8 * k + 8], 1, 0) for k in range(n)]
    inner = lax.broadcasted_iota(jnp.int32, turned[0].shape, 0) > 0
    joined = [jnp.where(inner, turned[k], turned[k - 1]) for k in range(1, n)]
    return jnp.concatenate([turned[0], *joined], axis=0)


def up_z(v):
    low, high = pltpu.roll(v[:, :128], 127, 1), pltpu.roll(v[:, 128:], 127, 1)
    inner = lax.broadcasted_iota(jnp.int32, low.shape, 1) < 127
    return jnp.concatenate([jnp.where(inner, low, high), jnp.where(inner, high, 0.0)], axis=1)


def dn_z(v, first=0.0):
    low, high = pltpu.roll(v[:, :128], 1, 1), pltpu.roll(v[:, 128:], 1, 1)
    inner = lax.broadcasted_iota(jnp.int32, low.shape, 1) > 0
    return jnp.concatenate([jnp.where(inner, low, first), jnp.where(inner, high, low)], axis=1)


def loop(low, high, compute, width=1):
    def group(x, count):
        for i in range(count):
            for ref, index, value in compute(x + i):
                ref[index] = value

    steps = (high - low) // width

    def step(k, carry):
        group(low + k * width, width)
        return carry

    lax.fori_loop(0, steps, step, 0)
    if (high - low) % width:
        group(low + steps * width, (high - low) % width)


def lookup(code, mats, rows):
    found = [jnp.zeros(code.shape, F32) for _ in rows]
    for m in range(8):
        hit = code == float(m + 1)
        found = [jnp.where(hit, mats[r, m], v) for r, v in zip(rows, found)]
    return found


def pack_x_kernel(ids, p, f, u, b, up_p, dn_p, up_m, dn_m, code, pv, fv, raw, sems):
    copies = []

    def take(src, dst):
        copies.append(pltpu.make_async_copy(src, dst, sems.at[len(copies)]))
        copies[-1].start()

    take(ids, raw)
    take(p, pv)
    take(f, fv)
    take(p.at[2:8], up_p.at[6:12])
    take(p.at[0:6], dn_p.at[6:12])
    take(f.at[3:8], up_p.at[12:17])
    take(f.at[0:5], dn_p.at[12:17])
    for a in range(3):
        take(u.at[a, 5:8], up_m.at[3 * a : 3 * a + 3])
        take(u.at[a, 0:4], dn_m.at[4 * a : 4 * a + 4])
        take(b.at[a, 6:8], up_m.at[9 + 2 * a : 11 + 2 * a])
        take(b.at[a, 0:3], dn_m.at[12 + 3 * a : 15 + 3 * a])
    copies[0].wait()
    for x in range(NX):
        c = (raw[x] + 1).astype(F32)
        code[x] = c
        if x >= 2:
            up_p[x - 2] = c
        if x < 6:
            dn_p[x] = c
    for copy in copies[1:]:
        copy.wait()


def pick(x, low, own, high, first, n_low):
    if x < n_low:
        return low, first[0] + x
    if x < n_low + NX:
        return own, x - n_low
    return high, first[1] + x - n_low - NX


def pack_y_pressure_kernel(ids, p, f, low, high, up, dn):
    for x in range(XE):
        ref, i = pick(x, low, ids, high, (0, 0), LOW)
        up[x] = ref[i, 8:16]
        dn[x] = ref[i, 0:8]
        ref, i = pick(x, low, p, high, (6, 6), LOW)
        up[20 + x] = ref[i, 8:16]
        dn[20 + x] = ref[i, 0:8]
    for x in range(XE - 2):
        ref, i = pick(x, low, f, high, (12, 12), LOW - 1)
        up[40 + x] = ref[i, 8:16]
        dn[40 + x] = ref[i, 0:8]


def pack_y_mech_kernel(u, b, low, high, up, dn):
    for a in range(3):
        for m in range(ME):
            ref, i = pick(m, low, u.at[a], high, (3 * a, 4 * a), ML)
            k, r = 8 * a + m // 2, 4 * (m % 2)
            up[k, r : r + 4] = ref[i, 12:16]
            dn[k, r : r + 4] = ref[i, 0:4]
        for m in range(ME - 2):
            ref, i = pick(m, low, b.at[a], high, (9 + 2 * a, 12 + 3 * a), ML - 1)
            k, r = 24 + 7 * a + m // 2, 4 * (m % 2)
            up[k, r : r + 4] = ref[i, 12:16]
            dn[k, r : r + 4] = ref[i, 0:4]


def masked(x, n_low, flags, v, lo, hi):
    if flags is None:
        return v, lo, hi
    lo, hi = (lo * flags[2], hi * flags[3])
    if n_low <= x < n_low + NX:
        return v, lo, hi
    edge = flags[0] if x < n_low else flags[1]
    return v * edge, lo * edge, hi * edge


def fill(out, n, n_low, own, low, high, first, yl, yh, k, flags):
    for x in range(n):
        ref, i = pick(x, low, own, high, first, n_low)
        v, lo, hi = masked(x, n_low, flags, ref[i], yl[k + x], yh[k + x])
        out[x, 8:24] = v
        out[x, 0:8] = lo
        out[x, 24:32] = hi


def fill_mech(out, n, n_low, own, low, high, first, yl, yh, k, flags, offset):
    for x in range(n):
        ref, i = pick(x, low, own, high, first, n_low)
        r = 4 * (x % 2)
        lo, hi = yl[k + x // 2, r : r + 4], yh[k + x // 2, r : r + 4]
        v, lo, hi = masked(x, n_low, flags, ref[i], lo, hi)
        out[x + offset, 0:4] = lo
        out[x + offset, 4:20] = v
        out[x + offset, 20:24] = hi


def two_sum(a, b):
    s = a + b
    t = s - a
    return s, (a - (s - t)) + (b - t)


def halves(a):
    c = 4097.0 * a
    high = c - (c - a)
    return high, a - high


def two_product(a, b):
    p = a * b
    (ah, al), (bh, bl) = halves(a), halves(b)
    return p, ((ah * bh - p) + ah * bl + al * bh) + al * bl


def dot(pairs, start, rest):
    for a, b in pairs:
        p, e = two_product(a, b)
        start, f = two_sum(start, p)
        rest = rest + (e + f)
    return start, rest


def solve(m):
    def minus(a, b):
        d, e = two_sum(a[0], 0.0 - b[0])
        return d, e + (a[1] - b[1])

    g00, g01, g02 = m[1], m[2], m[3]
    g11, g12, g22 = minus(m[2], m[3]), minus(m[3], m[4]), minus(m[4], m[5])
    right = (m[0], m[1], minus(m[1], m[2]))
    inverse = lambda d, scale: jnp.where(d > PIVOT * jnp.abs(scale), 1.0 / d, 0.0)
    i0 = inverse(g00[0], 0.0 * g00[0])
    l10, l20 = g01[0] * i0, g02[0] * i0
    i1 = inverse(g11[0] - l10 * g01[0], g11[0])
    e = g12[0] - l10 * g02[0]
    l21 = e * i1
    i2 = inverse(g22[0] - l20 * g02[0] - l21 * e, g22[0])

    def eliminate(c0, c1, c2):
        c1 = c1 - l10 * c0
        c2 = c2 - l20 * c0 - l21 * c1
        y2 = c2 * i2
        y1 = c1 * i1 - l21 * y2
        return c0 * i0 - l10 * y1 - l20 * y2, y1, y2

    y = eliminate(*[r[0] for r in right])
    left = []
    for r, row in zip(right, ((g00, g01, g02), (g01, g11, g12), (g02, g12, g22))):
        rest = r[1]
        for a, v in zip(row, y):
            rest = rest - a[1] * v
        d, rest = dot([(a[0], 0.0 - v) for a, v in zip(row, y)], r[0], rest)
        left.append(d + rest)
    return [a + b for a, b in zip(y, eliminate(*left))]


def coefficients(rows):
    high, low = two_sum(rows[0:64], rows[64:128])
    while high.shape[0] > 8:
        n = high.shape[0] // 2
        rest = low[:n] + low[n:]
        high, low = two_sum(high[:n], high[n:])
        low = low + rest
    for n in (4, 2, 1):
        rest = low + pltpu.roll(low, n, 0)
        high, low = two_sum(high, pltpu.roll(high, n, 0))
        low = low + rest
    spread = lambda v, k: jnp.broadcast_to(v[:, k : k + 1], (8, 128))
    at = lambda k: (spread(high, k), spread(low, k))
    y = solve([at(k) for k in range(6)])
    y = (y[0] + y[1], y[2] - y[1], 0.0 - y[2])
    c = (jnp.ones((8, 128), F32), *y)
    weights = [c[a] * c[b] * (1.0 if a == b else 2.0) for a, b in PAIRS]
    mu = []
    for k in range(6):
        terms = [at(6 + 10 * k + i) for i in range(len(PAIRS))]
        rest = 0.0
        for w, t in zip(weights, terms):
            rest = rest + w * t[1]
        mu.append(dot([(w, t[0]) for w, t in zip(weights, terms)], 0.0 * y[0], rest))
    v = solve(mu)
    scalar = lambda x: x[0, 0]
    return [scalar(x) for x in y], [[scalar(x * c[g]) for g in range(GENS)] for x in v]


def differences(v, x, cx, cy, cz):
    c = v[x]
    fy, fz = cy[x] * (c - up_y(c)), cz[x] * (c - up_z(c))
    return (
        cx[x] * (c - v[x + 1])
        + cx[x - 1] * (c - v[x - 1])
        + (fy - dn_y(fy))
        + (fz - dn_z(fz))
    )


def pressure_chain(source, p, cx, cy, cz, inv, total, t, n, k, part):
    def first(x):
        r = source(x) - differences(p, x, cx, cy, cz)
        return [(n, (0, x), r), (t, (0, x), inv[x] * r)]

    loop(1, XE - 1, first, PW)
    for i in (1, 2):

        def follow(x):
            c = t[i - 1, x]
            a = total[x] * c + differences(t.at[i - 1], x, cx, cy, cz)
            d = inv[x] * a
            return [(n, (i, x), a), (k, (i - 1, x), d), (t, (i, x), c - d)]

        loop(1 + i, XE - 1 - i, follow, PW)

    def final(x):
        v = k[1, x]
        e = cx[x] * k[1, x + 1] + cy[x] * up_y(v) + cz[x] * up_z(v)
        return [(n, (3, x), 2.0 * e)]

    loop(LOW, LOW + NX, final, PW)

    def body(x, acc):
        s = [v[LOW + x, 8:24] for v in (t.at[0], k.at[0], k.at[1])]
        q = [n[i, LOW + x, 8:24] for i in range(4)]
        return tuple(v + s[i] * q[j] for v, (i, j) in zip(acc, LEVELS))

    sums = lax.fori_loop(0, NX, body, (jnp.zeros((NY, NZ), F32),) * 6)
    at = lax.broadcasted_iota(jnp.int32, (8, 128), 1)
    row = jnp.zeros((8, 128), F32)
    for k, v in enumerate(sums):
        row = jnp.where(at == k, jnp.sum(v), row)
    part[...] = row


def pressure_first_kernel(
    flags, mats, ids, p, f, low, high, yl, yh,
    code, pe, coef, t, part,
    fe, perm, stor, n, k,
):
    cx, cy, cz, inv, stab, base, biot, total = (coef.at[i] for i in range(8))
    fill(code, XE, LOW, ids, low, high, (0, 0), yl, yh, 0, flags)
    fill(pe, XE, LOW, p, low, high, (6, 6), yl, yh, 20, flags)
    fill(fe.at[1 : XE - 1], XE - 2, LOW - 1, f, low, high, (12, 12), yl, yh, 40, None)

    def tables(x):
        l, s, k, st, bi = lookup(code[x], mats, range(5))
        bi = 0.25 * bi
        st2 = bi * bi / jnp.maximum(l + (2.0 / 3.0) * s, 1e-30)
        return [(perm, x, k), (stor, x, st), (biot, x, bi), (stab, x, st2)]

    loop(0, XE, tables)

    def faces(x):
        k = perm[x]

        def harmonic(other):
            return (2.0 * DT) * k * other / jnp.maximum(k + other, 1e-30)

        return [
            (cx, x, harmonic(perm[x + 1])),
            (cy, x, harmonic(up_y(k))),
            (cz, x, harmonic(up_z(k))),
        ]

    loop(0, XE - 1, faces, 2)

    def diagonal(x):
        y, z = cy[x], cz[x]
        flow = cx[x] + cx[x - 1] + y + dn_y(y) + z + dn_z(z)
        inside = code[x] > 0.5
        d = stor[x] + stab[x] + flow
        return [
            (inv, x, jnp.where(inside, 1.0 / jnp.where(inside, d, 1.0), 0.0)),
            (total, x, stor[x] + stab[x]),
            (base, x, stor[x] * pe[x] + DT * fe[x]),
        ]

    loop(1, XE - 1, diagonal, 2)
    pressure_chain(lambda x: DT * fe[x], pe, cx, cy, cz, inv, total, t, n, k, part)


def pressure_next_kernel(
    flags, coef, p, du, uo, low, high, yl, yh,
    pe, ue, t, part,
    de, n, k,
):
    cx, cy, cz, inv, stab, base, biot, total = (coef.at[i] for i in range(8))
    edge = lambda x, n: flags[0] if x < n else flags[1]
    zero = jnp.zeros((2, NZ), F32)
    for a in range(3):
        for x in range(19):
            j = 6 * (19 * a + x)
            out = de.at[a, x + 1]
            lo, hi = yl[j : j + 6] * flags[2], yh[j : j + 6] * flags[3]
            if 5 <= x < 14:
                out[4:28] = du[a, x - 5]
            else:
                outer = edge(x, 5)
                lo, hi = lo * outer, hi * outer
                ref = low.at[5 * a + x] if x < 5 else high.at[5 * a + x - 14]
                out[8:24] = ref[...] * outer
            if x == 13:
                lo, hi = lo * flags[1], hi * flags[1]
            out[0:2] = zero
            out[2:8] = lo
            out[24:30] = hi
            out[30:32] = zero
    for x in range(XE):
        j = 344 + 8 * x
        lo, hi = yl[j : j + 8] * flags[2], yh[j : j + 8] * flags[3]
        if not LOW <= x < LOW + NX:
            lo, hi = lo * edge(x, LOW), hi * edge(x, LOW)
        if 3 <= x < 17:
            pe[x, 8:24] = p[x - 3, 8:24]
        else:
            ref = low.at[15 + x] if x < 3 else high.at[15 + x - 17]
            pe[x, 8:24] = ref[...] * edge(x, LOW)
        pe[x, 0:8] = lo
        pe[x, 24:32] = hi

    def start(x):
        c2 = de[2, x]
        div = (
            (de[0, x + 1] - de[0, x])
            + (up_y(de[1, x]) - de[1, x])
            + (up_z(c2) - c2)
        )
        return base[x] - biot[x] * div + (stab[x] - total[x]) * pe[x]

    pressure_chain(start, pe, cx, cy, cz, inv, total, t, n, k, part)
    for a in range(3):
        for m in range(ME):
            ue[a, m] = uo[a, m] + de[a, m + MO, 4:28]


def mech_chain(u, bf, pe, t, biot, mc, kept, q, load, carry, acc, s, tg, part_p, part):
    sx, sy, sz, half, lame, h0, h1, h2, kk = (mc.at[i] for i in range(9))
    h = (h0, h1, h2)

    def loads(m):
        x = m + MO
        bi = biot[x, 4:28]
        fields = [pe[x, 4:28]] + [t[i, x, 4:28] for i in range(3)]
        return [(load, (g, m), bi * v) for g, v in enumerate(fields)]

    loop(0, ME - 1, loads, 2)

    def precondition(r, m):
        hs = [h[a][m] for a in range(3)]
        scaled = [r[a] * hs[a] for a in range(3)]
        k = kk[m] * (scaled[0] + scaled[1] + scaled[2])
        return [scaled[a] - hs[a] * k for a in range(3)]

    def apply(w, m, more, below):
        c = [w[a, m] for a in range(3)]
        d = (c[0] - w[0, m + 1], c[1] - up_y(c[1]), c[2] - up_z(c[2]))
        l = 0.0 - lame[m] * (d[0] + d[1] + d[2])
        if more is not None:
            l = l - more
        x, xb, y, z, g = sx[m], sx[m - 1], sy[m], sz[m], half[m, :, :128]

        def along_x(a):
            return x * (c[a] - w[a, m + 1]) + xb * (c[a] - w[a, m - 1])

        def along_y(a):
            f = y * (c[a] - up_y(c[a]))
            return f - dn_y(f)

        def along_z(a):
            f = z * (c[a] - up_z(c[a]))
            return f + dn_z(0.0 - f, g * c[a][:, :128])

        fx, fy, fz = x * d[0], y * d[1], z * d[2]
        r = [
            (fx + below - l) + along_y(0) + along_z(0),
            (fy + dn_y(l - fy) - l) + along_x(1) + along_z(1),
            (fz + dn_z(l - fz, g * c[2][:, :128]) - l) + along_x(2) + along_y(2),
        ]
        return r, l - fx

    def carried(w, m, more):
        c = [w[a, m] for a in range(3)]
        d = (c[0] - w[0, m + 1], c[1] - up_y(c[1]), c[2] - up_z(c[2]))
        l = 0.0 - lame[m] * (d[0] + d[1] + d[2])
        if more is not None:
            l = l - more
        return l - sx[m] * d[0]

    carry[0] = carried(u, 0, load[0, 0])

    def own(m):
        return jnp.where((m >= ML) & (m < ML + NX), m - ML, NX)

    def near(m):
        return jnp.where((m >= ML) & (m <= ML + NX), m - ML, NX + 1)

    def residual(m):
        for g in range(GENS):
            if g == 0:
                r, up = apply(u, m, load[0, m], carry[0])
                yield carry, 0, up
                r = [bf[a, m] - r[a] for a in range(3)]
            else:
                c = load[g, m]
                r = [load[g, m - 1] - c, dn_y(c) - c, dn_z(c) - c]
            z = precondition(r, m)
            for a in range(3):
                yield q, (0, g, a, own(m)), r[a]
                yield s, (0, g, a, m), z[a]
                yield kept, (g * 3 + a, near(m)), z[a]

    loop(1, ME - 1, residual, 2)

    for i in (1, 2):
        for g in range(GENS):
            carry[g] = carried(s.at[i - 1, g], i, None)

        def follow(m):
            for g in range(GENS):
                w = s.at[i - 1, g]
                r, up = apply(w, m, None, carry[g])
                yield carry, g, up
                v = precondition(r, m)
                for a in range(3):
                    yield q, (i, g, a, own(m)), r[a]
                    yield kept, ((i * GENS + g) * 3 + a, near(m)), v[a]
                    if i == 1:
                        yield s, (1, g, a, m), w[a, m] - v[a]

        loop(1 + i, ME - 1 - i, follow)

    def energy(m):
        l, x, y, z = lame[m], sx[m], sy[m], sz[m]
        low = (0.5 * lame[m - 1], 0.5 * dn_y(l), 0.5 * dn_z(l))
        for g in range(GENS):
            k = (2 * GENS + g) * 3
            w, o = kept.at[k : k + 3], ML
            total = 0.0
            for a in range(3):
                c = w[a, m - o]
                up = (w[a, m + 1 - o], up_y(c), up_z(c))
                total = total + up[a]
                yield q, (3, g, a, m - ML), x * up[0] + y * up[1] + z * up[2] + low[a] * c
            near_sum = w[0, m - o] + w[1, m - o] + w[2, m - o]
            yield tg, (0, g, m - ML), total
            yield tg, (1, g, m - ML), l * (near_sum - 0.5 * total)

    loop(ML, ML + NX, energy)

    top = lax.broadcasted_iota(jnp.int32, (8, NZ), 0) >= 4
    for k, (i, j) in enumerate(LEVELS):

        def body(step, sums):
            sums = list(sums)
            for x in (2 * step, 2 * step + 1):
                for a in range(3 if j < 3 else 4):
                    if a < 3:
                        v = [kept[(i * GENS + g) * 3 + a, x] for g in range(GENS)]
                        w = [q[j, g, a, x] for g in range(GENS)]
                    else:
                        v = [tg[0, g, x] for g in range(GENS)]
                        w = [tg[1, g, x] for g in range(GENS)]
                    for pick_rows in (
                        lambda f: f[8:16],
                        lambda f: jnp.where(top, f[0:8], f[16:24]),
                    ):
                        vt, wt = [pick_rows(f) for f in v], [pick_rows(f) for f in w]
                        sums = [c + vt[g] * wt[o] for c, (g, o) in zip(sums, PAIRS)]
                        if j == 3:
                            sums = [c + vt[o] * wt[g] for c, (g, o) in zip(sums, PAIRS)]
            return tuple(sums)

        sums = lax.fori_loop(0, NX // 2, body, (jnp.zeros((8, NZ), F32),) * len(PAIRS))
        for n, v in enumerate(sums):
            acc[10 * k + n] = v
    at = lax.broadcasted_iota(jnp.int32, (8, 128), 1)
    row = part_p[...]
    for k in range(60):
        row = jnp.where(at == k + 6, jnp.sum(acc[k]), row)
    for i in range(0, 128, 8):
        part[i : i + 8] = row


def mech_first_kernel(
    flags, mats, part_p, code, pe, coef, t, u, b, low, high, yl, yh,
    ue, be, mc, kept, part,
    q, load, shear, carry, acc, s, tg,
):
    sx, sy, sz, half, lame, h0, h1, h2, kk = (mc.at[i] for i in range(9))
    for a in range(3):
        fill_mech(ue.at[a], ME, ML, u.at[a], low, high, (3 * a, 4 * a), yl, yh, 8 * a, flags, 0)
        fill_mech(
            be.at[a], ME - 2, ML - 1, b.at[a], low, high, (9 + 2 * a, 12 + 3 * a), yl, yh, 24 + 7 * a, None, 1
        )

    def tables(m):
        l, g = lookup(code[m + MO, 4:28], mats, (0, 1))
        return [(lame, m, l), (shear, m, g)]

    loop(0, ME, tables)

    def faces(m):
        g = shear[m]
        return [
            (sx, m, 0.5 * (g + shear[m + 1])),
            (sy, m, 0.5 * (g + up_y(g))),
            (sz, m, 0.5 * (g + up_z(g))),
        ]

    loop(0, ME - 1, faces, 2)

    def diagonal(m):
        g, l = shear[m], lame[m]
        near = (
            shear[m + 1] + shear[m - 1] + up_y(g) + dn_y(g)
            + up_z(g) + dn_z(g)
        )
        d = 3.0 * g + 0.5 * near
        inside = g > 0.0
        lows = (lame[m - 1], dn_y(l), dn_z(l))
        hs = [jnp.where(inside, 1.0 / jnp.where(inside, d + v, 1.0), 0.0) for v in lows]
        k = l / (1.0 + l * (hs[0] + hs[1] + hs[2]))
        return [(half, m, 0.5 * g), (h0, m, hs[0]), (h1, m, hs[1]), (h2, m, hs[2]), (kk, m, k)]

    loop(1, ME - 1, diagonal, 2)
    mech_chain(ue, be, pe, t, coef.at[6], mc, kept, q, load, carry, acc, s, tg, part_p, part)


def mech_next_kernel(
    part_p, pe, coef, t, ue, be, mc,
    kept, part,
    q, load, carry, acc, s, tg,
):
    mech_chain(ue, be, pe, t, coef.at[6], mc, kept, q, load, carry, acc, s, tg, part_p, part)


def combine(v, kept, a, x):
    total = 0.0
    for i in range(3):
        for g in range(GENS):
            total = total + v[i][g] * kept[(i * GENS + g) * 3 + a, x]
    return total


def change_kernel(rows, t, pe, kept, u, du, pnew, unew, up, dn):
    y, v = coefficients(rows)
    for k in range(PK):
        x = k + MO
        w = pe[x] + (y[0] * t[0, x] + y[1] * t[1, x] + y[2] * t[2, x])
        pnew[k] = w
        i = k - ML
        if 2 <= i <= 4:
            up[13 + i] = w[8:24]
        if 3 <= i <= 5:
            dn[12 + i] = w[8:24]
    for a in range(3):
        for i in range(NX + 1):
            d = combine(v, kept, a, i)
            du[a, i] = d
            if i < NX:
                unew[a, i] = u[a, i] + d[4:20]
            if 3 <= i <= 7:
                up[5 * a + i - 3] = d[4:20]
            if 1 <= i <= 5:
                dn[5 * a + i - 1] = d[4:20]


def pack_change_kernel(du, p, low, high, up, dn):
    for a in range(3):
        for x in range(19):
            if x < 5:
                ref, r = low.at[5 * a + x], 0
            elif x < 14:
                ref, r = du.at[a, x - 5], 4
            else:
                ref, r = high.at[5 * a + x - 14], 0
            k = 6 * (19 * a + x)
            up[k : k + 6] = ref[r + 10 : r + 16]
            dn[k : k + 6] = ref[r : r + 6]
    for x in range(XE):
        if x < 3:
            ref, r = low.at[15 + x], 0
        elif x < 17:
            ref, r = p.at[x - 3], 8
        else:
            ref, r = high.at[15 + x - 17], 0
        k = 344 + 8 * x
        up[k : k + 8] = ref[r + 8 : r + 16]
        dn[k : k + 8] = ref[r : r + 8]


def finish_kernel(rows, t, p, kept, u, unew, pnew):
    y, v = coefficients(rows)
    for x in range(NX):
        k = x + LOW
        w = p[k, 8:24] + (y[0] * t[0, k, 8:24] + y[1] * t[1, k, 8:24] + y[2] * t[2, k, 8:24])
        pnew[x] = w
        for a in range(3):
            unew[a, x] = u[a, x] + combine(v, kept, a, x)[4:20]


def call(kernel, name, ins, outs, scratch=(), specs=None, cost=0, limit=12):
    return pl.pallas_call(
        kernel,
        name=name,
        out_shape=[jax.ShapeDtypeStruct(o, F32) for o in outs],
        in_specs=specs or [VM] * len(ins),
        out_specs=[VM] * len(outs),
        scratch_shapes=[pltpu.VMEM(s, F32) if isinstance(s, tuple) else s for s in scratch],
        compiler_params=pltpu.CompilerParams(vmem_limit_bytes=limit * 2**20),
        cost_estimate=pl.CostEstimate(flops=cost, bytes_accessed=0, transcendentals=0) if cost else None,
    )(*ins)


def neighbours(axis, size, up, dn):
    ring = [(i, (i + 1) % size) for i in range(size)]
    return lax.ppermute(up, axis, ring), lax.ppermute(dn, axis, [(b, a) for a, b in ring])


def gather_rows(part):
    return lax.all_to_all(part, ("gx", "gy"), 0, 0, tiled=True)


def on_device(gx_size, gy_size, u, p, b, f, ids, mats):
    gx, gy = lax.axis_index("gx"), lax.axis_index("gy")
    flags = jnp.stack([gx > 0, gx < gx_size - 1, gy > 0, gy < gy_size - 1]).astype(F32)
    wide, mech = (YE, NZ), (YM, NZ)
    up_p, dn_p, up_m, dn_m, own_code, own_p, own_f = call(
        pack_x_kernel,
        "pack_x",
        [pltpu.with_memory_space_constraint(v, pltpu.HBM) for v in (ids, p, f, u, b)],
        [(17, NY, NZ), (17, NY, NZ), (15, NY, NZ), (21, NY, NZ)] + [(NX, NY, NZ)] * 3,
        [pltpu.VMEM((NX, NY, NZ), jnp.int32), pltpu.SemaphoreType.DMA((19,))],
        [HB] * 5,
    )
    low_p, high_p = neighbours("gx", gx_size, up_p, dn_p)
    low_m, high_m = neighbours("gx", gx_size, up_m, dn_m)
    up, dn = call(
        pack_y_pressure_kernel, "pack_yp", (own_code, own_p, own_f, low_p, high_p), [(58, 8, NZ), (58, 8, NZ)], limit=4
    )
    yl_p, yh_p = neighbours("gy", gy_size, up, dn)
    up, dn = call(pack_y_mech_kernel, "pack_ym", (u, b, low_m, high_m), [(45, 8, NZ), (45, 8, NZ)], limit=4)
    yl_m, yh_m = neighbours("gy", gy_size, up, dn)
    code, pe, coef, t, part_p = call(
        pressure_first_kernel,
        "pressure_first",
        (flags, mats, own_code, own_p, own_f, low_p, high_p, yl_p, yh_p),
        [(XE, *wide), (XE, *wide), (8, XE, *wide), (3, XE, *wide), (8, 128)],
        [(XE, *wide)] * 3 + [(4, XE, *wide), (2, XE, *wide)],
        [SM, SM] + [VM] * 7,
        COST,
    )
    mech_scratch = [
        (4, GENS, 3, NX + 1, *mech),
        (GENS, ME, *mech),
        (GENS, *mech),
        (60, 8, NZ),
        (2, GENS, 3, ME, *mech),
        (2, GENS, NX, *mech),
    ]
    basis = (9 * GENS, NX + 2, *mech)
    ue, be, mc, s, part = call(
        mech_first_kernel,
        "mech_first",
        (flags, mats, part_p, code, pe, coef, t, u, b, low_m, high_m, yl_m, yh_m),
        [(3, ME, *mech), (3, ME, *mech), (9, ME, *mech), basis, (128, 128)],
        mech_scratch[:2] + [(ME, *mech)] + mech_scratch[2:],
        [SM, SM] + [VM] * 11,
        COST,
        26,
    )
    rows = gather_rows(part)
    du, p1, u1, up, dn = call(
        change_kernel,
        "change",
        (rows, t, pe, s, u),
        [(3, NX + 1, *mech), (PK, *wide), (3, NX, NY, NZ), (18, NY, NZ), (18, NY, NZ)],
    )
    low, high = neighbours("gx", gx_size, up, dn)
    up, dn = call(pack_change_kernel, "pack_change", (du, p1, low, high), [(504, NZ), (504, NZ)])
    yl, yh = neighbours("gy", gy_size, up, dn)
    pe, ue, t, part_p = call(
        pressure_next_kernel,
        "pressure_next",
        (flags, coef, p1, du, ue, low, high, yl, yh),
        [(XE, *wide), (3, ME, *mech), (3, XE, *wide), (8, 128)],
        [(3, XE, *wide), (4, XE, *wide), (2, XE, *wide)],
        [SM] + [VM] * 8,
        COST,
    )
    s, part = call(
        mech_next_kernel,
        "mech_next",
        (part_p, pe, coef, t, ue, be, mc),
        [basis, (128, 128)],
        mech_scratch,
        None,
        COST,
        26,
    )
    rows = gather_rows(part)
    u2, p2 = call(
        finish_kernel,
        "finish",
        (rows, t, pe, s, u1),
        [(3, NX, NY, NZ), (NX, NY, NZ)],
    )
    return u2, p2


def solution(mesh):
    body = functools.partial(on_device, mesh.shape["gx"], mesh.shape["gy"])
    field, vector = P("gx", "gy", None), P(None, "gx", "gy", None)
    return jax.shard_map(
        body,
        mesh=mesh,
        in_specs=(vector, field, vector, field, field, P()),
        out_specs=(vector, field),
        check_vma=False,
    )
```

```python
import functools

import jax
import jax.numpy as jnp
from jax import lax
from jax.experimental import pallas as pl
from jax.experimental.pallas import tpu as pltpu
from jax.sharding import PartitionSpec as P

F32 = jnp.float32
DT = 4.0
NX, NY, NZ = 8, 16, 256
YE = 32
YM = 24
GENS = 4
PAIRS = [(a, b) for a in range(GENS) for b in range(a, GENS)]
LEVELS = ((0, 0), (0, 1), (1, 1), (1, 2), (2, 2), (2, 3))
LOW, HIGH = 6, 6
XE = LOW + NX + HIGH
ML, MH = 3, 4
ME = ML + NX + MH
MO = LOW - ML
PK = 3 + NX + 3
PIVOT = 2e-7
PW = 4
COST = 200_000_000

VM = pl.BlockSpec(memory_space=pltpu.VMEM)
SM = pl.BlockSpec(memory_space=pltpu.SMEM)
HB = pl.BlockSpec(memory_space=pltpu.HBM)


def up_y(v):
    n = v.shape[0] // 8
    turned = [pltpu.roll(v[8 * k : 8 * k + 8], 7, 0) for k in range(n)]
    inner = lax.broadcasted_iota(jnp.int32, turned[0].shape, 0) < 7
    joined = [jnp.where(inner, turned[k], turned[k + 1]) for k in range(n - 1)]
    return jnp.concatenate([*joined, turned[n - 1]], axis=0)


def dn_y(v):
    n = v.shape[0] // 8
    turned = [pltpu.roll(v[8 * k : 8 * k + 8], 1, 0) for k in range(n)]
    inner = lax.broadcasted_iota(jnp.int32, turned[0].shape, 0) > 0
    joined = [jnp.where(inner, turned[k], turned[k - 1]) for k in range(1, n)]
    return jnp.concatenate([turned[0], *joined], axis=0)


def up_z(v):
    low, high = pltpu.roll(v[:, :128], 127, 1), pltpu.roll(v[:, 128:], 127, 1)
    inner = lax.broadcasted_iota(jnp.int32, low.shape, 1) < 127
    return jnp.concatenate([jnp.where(inner, low, high), jnp.where(inner, high, 0.0)], axis=1)


def dn_z(v, first=0.0):
    low, high = pltpu.roll(v[:, :128], 1, 1), pltpu.roll(v[:, 128:], 1, 1)
    inner = lax.broadcasted_iota(jnp.int32, low.shape, 1) > 0
    return jnp.concatenate([jnp.where(inner, low, first), jnp.where(inner, high, low)], axis=1)


def loop(low, high, compute, width=1):
    def group(x, count):
        for i in range(count):
            for ref, index, value in compute(x + i):
                ref[index] = value

    steps = (high - low) // width

    def step(k, carry):
        group(low + k * width, width)
        return carry

    lax.fori_loop(0, steps, step, 0)
    if (high - low) % width:
        group(low + steps * width, (high - low) % width)


def lookup(code, mats, rows):
    found = [jnp.zeros(code.shape, F32) for _ in rows]
    for m in range(8):
        hit = code == float(m + 1)
        found = [jnp.where(hit, mats[r, m], v) for r, v in zip(rows, found)]
    return found


def pack_x_kernel(ids, p, f, u, b, up_p, dn_p, up_m, dn_m, code, pv, fv, raw, sems):
    copies = []

    def take(src, dst):
        copies.append(pltpu.make_async_copy(src, dst, sems.at[len(copies)]))
        copies[-1].start()

    take(ids, raw)
    take(p, pv)
    take(f, fv)
    take(p.at[2:8], up_p.at[6:12])
    take(p.at[0:6], dn_p.at[6:12])
    take(f.at[3:8], up_p.at[12:17])
    take(f.at[0:5], dn_p.at[12:17])
    for a in range(3):
        take(u.at[a, 5:8], up_m.at[3 * a : 3 * a + 3])
        take(u.at[a, 0:4], dn_m.at[4 * a : 4 * a + 4])
        take(b.at[a, 6:8], up_m.at[9 + 2 * a : 11 + 2 * a])
        take(b.at[a, 0:3], dn_m.at[12 + 3 * a : 15 + 3 * a])
    copies[0].wait()
    for x in range(NX):
        c = (raw[x] + 1).astype(F32)
        code[x] = c
        if x >= 2:
            up_p[x - 2] = c
        if x < 6:
            dn_p[x] = c
    for copy in copies[1:]:
        copy.wait()


def pick(x, low, own, high, first, n_low):
    if x < n_low:
        return low, first[0] + x
    if x < n_low + NX:
        return own, x - n_low
    return high, first[1] + x - n_low - NX


def pack_y_pressure_kernel(ids, p, f, low, high, up, dn):
    def put(k, n, source):
        ref, i = source
        up[k : k + n] = ref[i, NY - n : NY]
        dn[k : k + n] = ref[i, 0:n]

    for x in range(XE):
        put(6 * x, 6, pick(x, low, ids, high, (0, 0), LOW))
        put(120 + 6 * x, 6, pick(x, low, p, high, (6, 6), LOW))
    for x in range(XE - 2):
        put(240 + 5 * x, 5, pick(x, low, f, high, (12, 12), LOW - 1))


def pack_y_mech_kernel(u, b, low, high, up, dn):
    def put(k, n, source):
        ref, i = source
        up[k : k + n] = ref[i, NY - n : NY]
        dn[k : k + n] = ref[i, 0:n]

    for a in range(3):
        for m in range(ME):
            put(4 * (ME * a + m), 4, pick(m, low, u.at[a], high, (3 * a, 4 * a), ML))
        for m in range(ME - 2):
            source = pick(m, low, b.at[a], high, (9 + 2 * a, 12 + 3 * a), ML - 1)
            put(180 + 3 * (13 * a + m), 3, source)


def masked(x, n_low, flags, v, lo, hi):
    if flags is None:
        return v, lo, hi
    lo, hi = (lo * flags[2], hi * flags[3])
    if n_low <= x < n_low + NX:
        return v, lo, hi
    edge = flags[0] if x < n_low else flags[1]
    return v * edge, lo * edge, hi * edge


def fill(out, n, n_low, own, low, high, first, yl, yh, k, flags, rows):
    zero = jnp.zeros((8 - rows, NZ), F32)
    for x in range(n):
        ref, i = pick(x, low, own, high, first, n_low)
        j = k + rows * x
        v, lo, hi = masked(x, n_low, flags, ref[i], yl[j : j + rows], yh[j : j + rows])
        out[x, 0 : 8 - rows] = zero
        out[x, 8 - rows : 8] = lo
        out[x, 8:24] = v
        out[x, 24 : 24 + rows] = hi
        out[x, 24 + rows : 32] = zero


def fill_mech(out, n, n_low, own, low, high, first, yl, yh, k, flags, offset, rows):
    for x in range(n):
        ref, i = pick(x, low, own, high, first, n_low)
        j = k + rows * x
        lo, hi = yl[j : j + rows], yh[j : j + rows]
        v, lo, hi = masked(x, n_low, flags, ref[i], lo, hi)
        y = x + offset
        if rows < 4:
            out[y, 0 : 4 - rows] = jnp.zeros((4 - rows, NZ), F32)
            out[y, 20 + rows : 24] = jnp.zeros((4 - rows, NZ), F32)
        out[y, 4 - rows : 4] = lo
        out[y, 4:20] = v
        out[y, 20 : 20 + rows] = hi


def two_sum(a, b):
    s = a + b
    t = s - a
    return s, (a - (s - t)) + (b - t)


def halves(a):
    c = 4097.0 * a
    high = c - (c - a)
    return high, a - high


def two_product(a, b):
    p = a * b
    (ah, al), (bh, bl) = halves(a), halves(b)
    return p, ((ah * bh - p) + ah * bl + al * bh) + al * bl


def dot(pairs, start, rest):
    for a, b in pairs:
        p, e = two_product(a, b)
        start, f = two_sum(start, p)
        rest = rest + (e + f)
    return start, rest


def solve(m):
    def minus(a, b):
        d, e = two_sum(a[0], 0.0 - b[0])
        return d, e + (a[1] - b[1])

    g00, g01, g02 = m[1], m[2], m[3]
    g11, g12, g22 = minus(m[2], m[3]), minus(m[3], m[4]), minus(m[4], m[5])
    right = (m[0], m[1], minus(m[1], m[2]))
    inverse = lambda d, scale: jnp.where(d > PIVOT * jnp.abs(scale), 1.0 / d, 0.0)
    i0 = inverse(g00[0], 0.0 * g00[0])
    l10, l20 = g01[0] * i0, g02[0] * i0
    i1 = inverse(g11[0] - l10 * g01[0], g11[0])
    e = g12[0] - l10 * g02[0]
    l21 = e * i1
    i2 = inverse(g22[0] - l20 * g02[0] - l21 * e, g22[0])

    def eliminate(c0, c1, c2):
        c1 = c1 - l10 * c0
        c2 = c2 - l20 * c0 - l21 * c1
        y2 = c2 * i2
        y1 = c1 * i1 - l21 * y2
        return c0 * i0 - l10 * y1 - l20 * y2, y1, y2

    y = eliminate(*[r[0] for r in right])
    left = []
    for r, row in zip(right, ((g00, g01, g02), (g01, g11, g12), (g02, g12, g22))):
        rest = r[1]
        for a, v in zip(row, y):
            rest = rest - a[1] * v
        d, rest = dot([(a[0], 0.0 - v) for a, v in zip(row, y)], r[0], rest)
        left.append(d + rest)
    return [a + b for a, b in zip(y, eliminate(*left))]


def coefficients(rows):
    high, low = two_sum(rows[0:64], rows[64:128])
    while high.shape[0] > 8:
        n = high.shape[0] // 2
        rest = low[:n] + low[n:]
        high, low = two_sum(high[:n], high[n:])
        low = low + rest
    for n in (4, 2, 1):
        rest = low + pltpu.roll(low, n, 0)
        high, low = two_sum(high, pltpu.roll(high, n, 0))
        low = low + rest
    spread = lambda v, k: jnp.broadcast_to(v[:, k : k + 1], (8, 128))
    at = lambda k: (spread(high, k), spread(low, k))
    y = solve([at(k) for k in range(6)])
    y = (y[0] + y[1], y[2] - y[1], 0.0 - y[2])
    c = (jnp.ones((8, 128), F32), *y)
    weights = [c[a] * c[b] * (1.0 if a == b else 2.0) for a, b in PAIRS]
    mu = []
    for k in range(6):
        terms = [at(6 + 10 * k + i) for i in range(len(PAIRS))]
        rest = 0.0
        for w, t in zip(weights, terms):
            rest = rest + w * t[1]
        mu.append(dot([(w, t[0]) for w, t in zip(weights, terms)], 0.0 * y[0], rest))
    v = solve(mu)
    scalar = lambda x: x[0, 0]
    return [scalar(x) for x in y], [[scalar(x * c[g]) for g in range(GENS)] for x in v]


def differences(v, x, cx, cy, cz):
    c = v[x]
    fy, fz = cy[x] * (c - up_y(c)), cz[x] * (c - up_z(c))
    return (
        cx[x] * (c - v[x + 1])
        + cx[x - 1] * (c - v[x - 1])
        + (fy - dn_y(fy))
        + (fz - dn_z(fz))
    )


def pressure_chain(source, p, cx, cy, cz, inv, total, t, n, k, part):
    def first(x):
        r = source(x) - differences(p, x, cx, cy, cz)
        return [(n, (0, x), r), (t, (0, x), inv[x] * r)]

    loop(1, XE - 1, first, PW)
    for i in (1, 2):

        def follow(x):
            c = t[i - 1, x]
            a = total[x] * c + differences(t.at[i - 1], x, cx, cy, cz)
            d = inv[x] * a
            return [(n, (i, x), a), (k, (i - 1, x), d), (t, (i, x), c - d)]

        loop(1 + i, XE - 1 - i, follow, PW)

    def final(x):
        v = k[1, x]
        e = cx[x] * k[1, x + 1] + cy[x] * up_y(v) + cz[x] * up_z(v)
        return [(n, (3, x), 2.0 * e)]

    loop(LOW, LOW + NX, final, PW)

    def body(x, acc):
        s = [v[LOW + x, 8:24] for v in (t.at[0], k.at[0], k.at[1])]
        q = [n[i, LOW + x, 8:24] for i in range(4)]
        return tuple(v + s[i] * q[j] for v, (i, j) in zip(acc, LEVELS))

    sums = lax.fori_loop(0, NX, body, (jnp.zeros((NY, NZ), F32),) * 6)
    at = lax.broadcasted_iota(jnp.int32, (8, 128), 1)
    row = jnp.zeros((8, 128), F32)
    for k, v in enumerate(sums):
        row = jnp.where(at == k, jnp.sum(v), row)
    part[...] = row


def pressure_first_kernel(
    flags, mats, ids, p, f, low, high, yl, yh,
    code, pe, coef, t, part,
    fe, perm, stor, n, k,
):
    cx, cy, cz, inv, stab, base, biot, total = (coef.at[i] for i in range(8))
    fill(code, XE, LOW, ids, low, high, (0, 0), yl, yh, 0, flags, 6)
    fill(pe, XE, LOW, p, low, high, (6, 6), yl, yh, 120, flags, 6)
    fill(fe.at[1 : XE - 1], XE - 2, LOW - 1, f, low, high, (12, 12), yl, yh, 240, None, 5)

    def tables(x):
        l, s, k, st, bi = lookup(code[x], mats, range(5))
        bi = 0.25 * bi
        st2 = bi * bi / jnp.maximum(l + (2.0 / 3.0) * s, 1e-30)
        return [(perm, x, k), (stor, x, st), (biot, x, bi), (stab, x, st2)]

    loop(0, XE, tables)

    def faces(x):
        k = perm[x]

        def harmonic(other):
            return (2.0 * DT) * k * other / jnp.maximum(k + other, 1e-30)

        return [
            (cx, x, harmonic(perm[x + 1])),
            (cy, x, harmonic(up_y(k))),
            (cz, x, harmonic(up_z(k))),
        ]

    loop(0, XE - 1, faces, 2)

    def diagonal(x):
        y, z = cy[x], cz[x]
        flow = cx[x] + cx[x - 1] + y + dn_y(y) + z + dn_z(z)
        inside = code[x] > 0.5
        d = stor[x] + stab[x] + flow
        return [
            (inv, x, jnp.where(inside, 1.0 / jnp.where(inside, d, 1.0), 0.0)),
            (total, x, stor[x] + stab[x]),
            (base, x, stor[x] * pe[x] + DT * fe[x]),
        ]

    loop(1, XE - 1, diagonal, 2)
    pressure_chain(lambda x: DT * fe[x], pe, cx, cy, cz, inv, total, t, n, k, part)


def pressure_next_kernel(
    flags, coef, p, du, uo, low, high, yl, yh,
    pe, ue, t, part,
    de, n, k,
):
    cx, cy, cz, inv, stab, base, biot, total = (coef.at[i] for i in range(8))
    edge = lambda x, n: flags[0] if x < n else flags[1]
    zero = jnp.zeros((2, NZ), F32)
    for a in range(3):
        for x in range(19):
            j = 6 * (19 * a + x)
            out = de.at[a, x + 1]
            lo, hi = yl[j : j + 6] * flags[2], yh[j : j + 6] * flags[3]
            if 5 <= x < 14:
                out[4:28] = du[a, x - 5]
            else:
                outer = edge(x, 5)
                lo, hi = lo * outer, hi * outer
                ref = low.at[5 * a + x] if x < 5 else high.at[5 * a + x - 14]
                out[8:24] = ref[...] * outer
            if x == 13:
                lo, hi = lo * flags[1], hi * flags[1]
            out[0:2] = zero
            out[2:8] = lo
            out[24:30] = hi
            out[30:32] = zero
    for x in range(XE):
        j = 342 + 6 * x
        lo, hi = yl[j : j + 6] * flags[2], yh[j : j + 6] * flags[3]
        if not LOW <= x < LOW + NX:
            lo, hi = lo * edge(x, LOW), hi * edge(x, LOW)
        if 3 <= x < 17:
            pe[x, 8:24] = p[x - 3, 8:24]
        else:
            ref = low.at[15 + x] if x < 3 else high.at[15 + x - 17]
            pe[x, 8:24] = ref[...] * edge(x, LOW)
        pe[x, 0:2] = zero
        pe[x, 2:8] = lo
        pe[x, 24:30] = hi
        pe[x, 30:32] = zero

    def start(x):
        c2 = de[2, x]
        div = (
            (de[0, x + 1] - de[0, x])
            + (up_y(de[1, x]) - de[1, x])
            + (up_z(c2) - c2)
        )
        return base[x] - biot[x] * div + (stab[x] - total[x]) * pe[x]

    pressure_chain(start, pe, cx, cy, cz, inv, total, t, n, k, part)
    for a in range(3):
        for m in range(ME):
            ue[a, m] = uo[a, m] + de[a, m + MO, 4:28]


def mech_chain(u, bf, pe, t, biot, mc, kept, q, load, carry, acc, s, tg, part_p, part):
    sx, sy, sz, half, lame, h0, h1, h2, kk = (mc.at[i] for i in range(9))
    h = (h0, h1, h2)

    def loads(m):
        x = m + MO
        bi = biot[x, 4:28]
        fields = [pe[x, 4:28]] + [t[i, x, 4:28] for i in range(3)]
        return [(load, (g, m), bi * v) for g, v in enumerate(fields)]

    loop(0, ME - 1, loads, 2)

    def precondition(r, m):
        hs = [h[a][m] for a in range(3)]
        scaled = [r[a] * hs[a] for a in range(3)]
        k = kk[m] * (scaled[0] + scaled[1] + scaled[2])
        return [scaled[a] - hs[a] * k for a in range(3)]

    def apply(w, m, more, below):
        c = [w[a, m] for a in range(3)]
        d = (c[0] - w[0, m + 1], c[1] - up_y(c[1]), c[2] - up_z(c[2]))
        l = 0.0 - lame[m] * (d[0] + d[1] + d[2])
        if more is not None:
            l = l - more
        x, xb, y, z, g = sx[m], sx[m - 1], sy[m], sz[m], half[m, :, :128]

        def along_x(a):
            return x * (c[a] - w[a, m + 1]) + xb * (c[a] - w[a, m - 1])

        def along_y(a):
            f = y * (c[a] - up_y(c[a]))
            return f - dn_y(f)

        def along_z(a):
            f = z * (c[a] - up_z(c[a]))
            return f + dn_z(0.0 - f, g * c[a][:, :128])

        fx, fy, fz = x * d[0], y * d[1], z * d[2]
        r = [
            (fx + below - l) + along_y(0) + along_z(0),
            (fy + dn_y(l - fy) - l) + along_x(1) + along_z(1),
            (fz + dn_z(l - fz, g * c[2][:, :128]) - l) + along_x(2) + along_y(2),
        ]
        return r, l - fx

    def carried(w, m, more):
        c = [w[a, m] for a in range(3)]
        d = (c[0] - w[0, m + 1], c[1] - up_y(c[1]), c[2] - up_z(c[2]))
        l = 0.0 - lame[m] * (d[0] + d[1] + d[2])
        if more is not None:
            l = l - more
        return l - sx[m] * d[0]

    carry[0] = carried(u, 0, load[0, 0])

    def own(m):
        return jnp.where((m >= ML) & (m < ML + NX), m - ML, NX)

    def near(m):
        return jnp.where((m >= ML) & (m <= ML + NX), m - ML, NX + 1)

    def residual(m):
        for g in range(GENS):
            if g == 0:
                r, up = apply(u, m, load[0, m], carry[0])
                yield carry, 0, up
                r = [bf[a, m] - r[a] for a in range(3)]
            else:
                c = load[g, m]
                r = [load[g, m - 1] - c, dn_y(c) - c, dn_z(c) - c]
            z = precondition(r, m)
            for a in range(3):
                yield q, (0, g, a, own(m)), r[a]
                yield s, (0, g, a, m), z[a]
                yield kept, (g * 3 + a, near(m)), z[a]

    loop(1, ME - 1, residual, 2)

    for i in (1, 2):
        for g in range(GENS):
            carry[g] = carried(s.at[i - 1, g], i, None)

        def follow(m):
            for g in range(GENS):
                w = s.at[i - 1, g]
                r, up = apply(w, m, None, carry[g])
                yield carry, g, up
                v = precondition(r, m)
                for a in range(3):
                    yield q, (i, g, a, own(m)), r[a]
                    yield kept, ((i * GENS + g) * 3 + a, near(m)), v[a]
                    if i == 1:
                        yield s, (1, g, a, m), w[a, m] - v[a]

        loop(1 + i, ME - 1 - i, follow)

    def energy(m):
        l, x, y, z = lame[m], sx[m], sy[m], sz[m]
        low = (0.5 * lame[m - 1], 0.5 * dn_y(l), 0.5 * dn_z(l))
        for g in range(GENS):
            k = (2 * GENS + g) * 3
            w, o = kept.at[k : k + 3], ML
            total = 0.0
            for a in range(3):
                c = w[a, m - o]
                up = (w[a, m + 1 - o], up_y(c), up_z(c))
                total = total + up[a]
                yield q, (3, g, a, m - ML), x * up[0] + y * up[1] + z * up[2] + low[a] * c
            near_sum = w[0, m - o] + w[1, m - o] + w[2, m - o]
            yield tg, (0, g, m - ML), total
            yield tg, (1, g, m - ML), l * (near_sum - 0.5 * total)

    loop(ML, ML + NX, energy)

    top = lax.broadcasted_iota(jnp.int32, (8, NZ), 0) >= 4
    for k, (i, j) in enumerate(LEVELS):

        def body(step, sums):
            sums = list(sums)
            for x in (2 * step, 2 * step + 1):
                for a in range(3 if j < 3 else 4):
                    if a < 3:
                        v = [kept[(i * GENS + g) * 3 + a, x] for g in range(GENS)]
                        w = [q[j, g, a, x] for g in range(GENS)]
                    else:
                        v = [tg[0, g, x] for g in range(GENS)]
                        w = [tg[1, g, x] for g in range(GENS)]
                    for pick_rows in (
                        lambda f: f[8:16],
                        lambda f: jnp.where(top, f[0:8], f[16:24]),
                    ):
                        vt, wt = [pick_rows(f) for f in v], [pick_rows(f) for f in w]
                        sums = [c + vt[g] * wt[o] for c, (g, o) in zip(sums, PAIRS)]
                        if j == 3:
                            sums = [c + vt[o] * wt[g] for c, (g, o) in zip(sums, PAIRS)]
            return tuple(sums)

        sums = lax.fori_loop(0, NX // 2, body, (jnp.zeros((8, NZ), F32),) * len(PAIRS))
        for n, v in enumerate(sums):
            acc[10 * k + n] = v
    at = lax.broadcasted_iota(jnp.int32, (8, 128), 1)
    row = part_p[...]
    for k in range(60):
        row = jnp.where(at == k + 6, jnp.sum(acc[k]), row)
    for i in range(0, 128, 8):
        part[i : i + 8] = row


def mech_first_kernel(
    flags, mats, part_p, code, pe, coef, t, u, b, low, high, yl, yh,
    ue, be, mc, kept, part,
    q, load, shear, carry, acc, s, tg,
):
    sx, sy, sz, half, lame, h0, h1, h2, kk = (mc.at[i] for i in range(9))
    for a in range(3):
        fill_mech(ue.at[a], ME, ML, u.at[a], low, high, (3 * a, 4 * a), yl, yh, 60 * a, flags, 0, 4)
        fill_mech(
            be.at[a], ME - 2, ML - 1, b.at[a], low, high, (9 + 2 * a, 12 + 3 * a), yl, yh, 180 + 39 * a, None, 1, 3
        )

    def tables(m):
        l, g = lookup(code[m + MO, 4:28], mats, (0, 1))
        return [(lame, m, l), (shear, m, g)]

    loop(0, ME, tables)

    def faces(m):
        g = shear[m]
        return [
            (sx, m, 0.5 * (g + shear[m + 1])),
            (sy, m, 0.5 * (g + up_y(g))),
            (sz, m, 0.5 * (g + up_z(g))),
        ]

    loop(0, ME - 1, faces, 2)

    def diagonal(m):
        g, l = shear[m], lame[m]
        near = (
            shear[m + 1] + shear[m - 1] + up_y(g) + dn_y(g)
            + up_z(g) + dn_z(g)
        )
        d = 3.0 * g + 0.5 * near
        inside = g > 0.0
        lows = (lame[m - 1], dn_y(l), dn_z(l))
        hs = [jnp.where(inside, 1.0 / jnp.where(inside, d + v, 1.0), 0.0) for v in lows]
        k = l / (1.0 + l * (hs[0] + hs[1] + hs[2]))
        return [(half, m, 0.5 * g), (h0, m, hs[0]), (h1, m, hs[1]), (h2, m, hs[2]), (kk, m, k)]

    loop(1, ME - 1, diagonal, 2)
    mech_chain(ue, be, pe, t, coef.at[6], mc, kept, q, load, carry, acc, s, tg, part_p, part)


def mech_next_kernel(
    part_p, pe, coef, t, ue, be, mc,
    kept, part,
    q, load, carry, acc, s, tg,
):
    mech_chain(ue, be, pe, t, coef.at[6], mc, kept, q, load, carry, acc, s, tg, part_p, part)


def combine(v, kept, a, x):
    total = 0.0
    for i in range(3):
        for g in range(GENS):
            total = total + v[i][g] * kept[(i * GENS + g) * 3 + a, x]
    return total


def change_kernel(rows, t, pe, kept, u, du, pnew, unew, up, dn):
    y, v = coefficients(rows)
    for k in range(PK):
        x = k + MO
        w = pe[x] + (y[0] * t[0, x] + y[1] * t[1, x] + y[2] * t[2, x])
        pnew[k] = w
        i = k - ML
        if 2 <= i <= 4:
            up[13 + i] = w[8:24]
        if 3 <= i <= 5:
            dn[12 + i] = w[8:24]
    for a in range(3):
        for i in range(NX + 1):
            d = combine(v, kept, a, i)
            du[a, i] = d
            if i < NX:
                unew[a, i] = u[a, i] + d[4:20]
            if 3 <= i <= 7:
                up[5 * a + i - 3] = d[4:20]
            if 1 <= i <= 5:
                dn[5 * a + i - 1] = d[4:20]


def pack_change_kernel(du, p, low, high, up, dn):
    for a in range(3):
        for x in range(19):
            if x < 5:
                ref, r = low.at[5 * a + x], 0
            elif x < 14:
                ref, r = du.at[a, x - 5], 4
            else:
                ref, r = high.at[5 * a + x - 14], 0
            k = 6 * (19 * a + x)
            up[k : k + 6] = ref[r + 10 : r + 16]
            dn[k : k + 6] = ref[r : r + 6]
    for x in range(XE):
        if x < 3:
            ref, r = low.at[15 + x], 0
        elif x < 17:
            ref, r = p.at[x - 3], 8
        else:
            ref, r = high.at[15 + x - 17], 0
        k = 342 + 6 * x
        up[k : k + 6] = ref[r + 10 : r + 16]
        dn[k : k + 6] = ref[r : r + 6]


def finish_kernel(rows, t, p, kept, u, unew, pnew):
    y, v = coefficients(rows)
    for x in range(NX):
        k = x + LOW
        w = p[k, 8:24] + (y[0] * t[0, k, 8:24] + y[1] * t[1, k, 8:24] + y[2] * t[2, k, 8:24])
        pnew[x] = w
        for a in range(3):
            unew[a, x] = u[a, x] + combine(v, kept, a, x)[4:20]


def call(kernel, name, ins, outs, scratch=(), specs=None, cost=0, limit=12):
    return pl.pallas_call(
        kernel,
        name=name,
        out_shape=[jax.ShapeDtypeStruct(o, F32) for o in outs],
        in_specs=specs or [VM] * len(ins),
        out_specs=[VM] * len(outs),
        scratch_shapes=[pltpu.VMEM(s, F32) if isinstance(s, tuple) else s for s in scratch],
        compiler_params=pltpu.CompilerParams(vmem_limit_bytes=limit * 2**20),
        cost_estimate=pl.CostEstimate(flops=cost, bytes_accessed=0, transcendentals=0) if cost else None,
    )(*ins)


def neighbours(axis, size, up, dn):
    ring = [(i, (i + 1) % size) for i in range(size)]
    return lax.ppermute(up, axis, ring), lax.ppermute(dn, axis, [(b, a) for a, b in ring])


def gather_rows(part):
    return lax.all_to_all(part, ("gx", "gy"), 0, 0, tiled=True)


def on_device(gx_size, gy_size, u, p, b, f, ids, mats):
    gx, gy = lax.axis_index("gx"), lax.axis_index("gy")
    flags = jnp.stack([gx > 0, gx < gx_size - 1, gy > 0, gy < gy_size - 1]).astype(F32)
    wide, mech = (YE, NZ), (YM, NZ)
    up_p, dn_p, up_m, dn_m, own_code, own_p, own_f = call(
        pack_x_kernel,
        "pack_x",
        [pltpu.with_memory_space_constraint(v, pltpu.HBM) for v in (ids, p, f, u, b)],
        [(17, NY, NZ), (17, NY, NZ), (15, NY, NZ), (21, NY, NZ)] + [(NX, NY, NZ)] * 3,
        [pltpu.VMEM((NX, NY, NZ), jnp.int32), pltpu.SemaphoreType.DMA((19,))],
        [HB] * 5,
    )
    low_p, high_p = neighbours("gx", gx_size, up_p, dn_p)
    low_m, high_m = neighbours("gx", gx_size, up_m, dn_m)
    up, dn = call(
        pack_y_pressure_kernel, "pack_yp", (own_code, own_p, own_f, low_p, high_p), [(336, NZ), (336, NZ)], limit=4
    )
    yl_p, yh_p = neighbours("gy", gy_size, up, dn)
    up, dn = call(pack_y_mech_kernel, "pack_ym", (u, b, low_m, high_m), [(304, NZ), (304, NZ)], limit=4)
    yl_m, yh_m = neighbours("gy", gy_size, up, dn)
    code, pe, coef, t, part_p = call(
        pressure_first_kernel,
        "pressure_first",
        (flags, mats, own_code, own_p, own_f, low_p, high_p, yl_p, yh_p),
        [(XE, *wide), (XE, *wide), (8, XE, *wide), (3, XE, *wide), (8, 128)],
        [(XE, *wide)] * 3 + [(4, XE, *wide), (2, XE, *wide)],
        [SM, SM] + [VM] * 7,
        2_000_000_000,
    )
    mech_scratch = [
        (4, GENS, 3, NX + 1, *mech),
        (GENS, ME, *mech),
        (GENS, *mech),
        (60, 8, NZ),
        (2, GENS, 3, ME, *mech),
        (2, GENS, NX, *mech),
    ]
    basis = (9 * GENS, NX + 2, *mech)
    ue, be, mc, s, part = call(
        mech_first_kernel,
        "mech_first",
        (flags, mats, part_p, code, pe, coef, t, u, b, low_m, high_m, yl_m, yh_m),
        [(3, ME, *mech), (3, ME, *mech), (9, ME, *mech), basis, (128, 128)],
        mech_scratch[:2] + [(ME, *mech)] + mech_scratch[2:],
        [SM, SM] + [VM] * 11,
        COST,
        26,
    )
    rows = gather_rows(part)
    du, p1, u1, up, dn = call(
        change_kernel,
        "change",
        (rows, t, pe, s, u),
        [(3, NX + 1, *mech), (PK, *wide), (3, NX, NY, NZ), (18, NY, NZ), (18, NY, NZ)],
    )
    low, high = neighbours("gx", gx_size, up, dn)
    up, dn = call(pack_change_kernel, "pack_change", (du, p1, low, high), [(464, NZ), (464, NZ)])
    yl, yh = neighbours("gy", gy_size, up, dn)
    pe, ue, t, part_p = call(
        pressure_next_kernel,
        "pressure_next",
        (flags, coef, p1, du, ue, low, high, yl, yh),
        [(XE, *wide), (3, ME, *mech), (3, XE, *wide), (8, 128)],
        [(3, XE, *wide), (4, XE, *wide), (2, XE, *wide)],
        [SM] + [VM] * 8,
        COST,
    )
    s, part = call(
        mech_next_kernel,
        "mech_next",
        (part_p, pe, coef, t, ue, be, mc),
        [basis, (128, 128)],
        mech_scratch,
        None,
        COST,
        26,
    )
    rows = gather_rows(part)
    u2, p2 = call(
        finish_kernel,
        "finish",
        (rows, t, pe, s, u1),
        [(3, NX, NY, NZ), (NX, NY, NZ)],
    )
    return u2, p2


def solution(mesh):
    body = functools.partial(on_device, mesh.shape["gx"], mesh.shape["gy"])
    field, vector = P("gx", "gy", None), P(None, "gx", "gy", None)
    return jax.shard_map(
        body,
        mesh=mesh,
        in_specs=(vector, field, vector, field, field, P()),
        out_specs=(vector, field),
        check_vma=False,
    )
```

```python
import functools

import jax
import jax.numpy as jnp
from jax import lax
from jax.experimental import pallas as pl
from jax.experimental.pallas import tpu as pltpu
from jax.sharding import PartitionSpec as P

F32 = jnp.float32
DT = 4.0
NX, NY, NZ = 8, 16, 256
YE = 32
YM = 24
GENS = 4
PAIRS = [(a, b) for a in range(GENS) for b in range(a, GENS)]
LEVELS = ((0, 0), (0, 1), (1, 1), (1, 2), (2, 2), (2, 3))
LOW, HIGH = 6, 6
XE = LOW + NX + HIGH
ML, MH = 3, 4
ME = ML + NX + MH
MO = LOW - ML
PK = 3 + NX + 3
PIVOT = 2e-7
PW = 4
COST = 200_000_000

VM = pl.BlockSpec(memory_space=pltpu.VMEM)
SM = pl.BlockSpec(memory_space=pltpu.SMEM)
HB = pl.BlockSpec(memory_space=pltpu.HBM)


def up_y(v):
    n = v.shape[0] // 8
    turned = [pltpu.roll(v[8 * k : 8 * k + 8], 7, 0) for k in range(n)]
    inner = lax.broadcasted_iota(jnp.int32, turned[0].shape, 0) < 7
    joined = [jnp.where(inner, turned[k], turned[k + 1]) for k in range(n - 1)]
    return jnp.concatenate([*joined, turned[n - 1]], axis=0)


def dn_y(v):
    n = v.shape[0] // 8
    turned = [pltpu.roll(v[8 * k : 8 * k + 8], 1, 0) for k in range(n)]
    inner = lax.broadcasted_iota(jnp.int32, turned[0].shape, 0) > 0
    joined = [jnp.where(inner, turned[k], turned[k - 1]) for k in range(1, n)]
    return jnp.concatenate([turned[0], *joined], axis=0)


def up_z(v):
    low, high = pltpu.roll(v[:, :128], 127, 1), pltpu.roll(v[:, 128:], 127, 1)
    inner = lax.broadcasted_iota(jnp.int32, low.shape, 1) < 127
    return jnp.concatenate([jnp.where(inner, low, high), jnp.where(inner, high, 0.0)], axis=1)


def dn_z(v, first=0.0):
    low, high = pltpu.roll(v[:, :128], 1, 1), pltpu.roll(v[:, 128:], 1, 1)
    inner = lax.broadcasted_iota(jnp.int32, low.shape, 1) > 0
    return jnp.concatenate([jnp.where(inner, low, first), jnp.where(inner, high, low)], axis=1)


def loop(low, high, compute, width=1):
    def group(x, count):
        for i in range(count):
            for ref, index, value in compute(x + i):
                ref[index] = value

    steps = (high - low) // width

    def step(k, carry):
        group(low + k * width, width)
        return carry

    lax.fori_loop(0, steps, step, 0)
    if (high - low) % width:
        group(low + steps * width, (high - low) % width)


def lookup(code, mats, rows):
    found = [jnp.zeros(code.shape, F32) for _ in rows]
    for m in range(8):
        hit = code == float(m + 1)
        found = [jnp.where(hit, mats[r, m], v) for r, v in zip(rows, found)]
    return found


def fetcher(sems):
    copies = []

    def take(src, dst):
        copies.append(pltpu.make_async_copy(src, dst, sems.at[len(copies)]))
        copies[-1].start()

    return copies, take


def pack_x_pressure_kernel(ids, p, f, up, dn, code, pv, fv, raw, sems):
    copies, take = fetcher(sems)
    take(ids, raw)
    take(p, pv)
    take(f, fv)
    take(p.at[2:8], up.at[6:12])
    take(p.at[0:6], dn.at[6:12])
    take(f.at[3:8], up.at[12:17])
    take(f.at[0:5], dn.at[12:17])
    copies[0].wait()
    for x in range(NX):
        c = (raw[x] + 1).astype(F32)
        code[x] = c
        if x >= 2:
            up[x - 2] = c
        if x < 6:
            dn[x] = c
    for copy in copies[1:]:
        copy.wait()


def pack_x_mech_kernel(u, b, after, up, dn, sems):
    del after
    copies, take = fetcher(sems)
    for a in range(3):
        take(u.at[a, 5:8], up.at[3 * a : 3 * a + 3])
        take(u.at[a, 0:4], dn.at[4 * a : 4 * a + 4])
        take(b.at[a, 6:8], up.at[9 + 2 * a : 11 + 2 * a])
        take(b.at[a, 0:3], dn.at[12 + 3 * a : 15 + 3 * a])
    for copy in copies:
        copy.wait()


def pick(x, low, own, high, first, n_low):
    if x < n_low:
        return low, first[0] + x
    if x < n_low + NX:
        return own, x - n_low
    return high, first[1] + x - n_low - NX


def pack_y_pressure_kernel(ids, p, f, low, high, up, dn):
    def put(k, n, source):
        ref, i = source
        up[k : k + n] = ref[i, NY - n : NY]
        dn[k : k + n] = ref[i, 0:n]

    for x in range(XE):
        put(6 * x, 6, pick(x, low, ids, high, (0, 0), LOW))
        put(120 + 6 * x, 6, pick(x, low, p, high, (6, 6), LOW))
    for x in range(XE - 2):
        put(240 + 5 * x, 5, pick(x, low, f, high, (12, 12), LOW - 1))


def pack_y_mech_kernel(u, b, low, high, up, dn):
    def put(k, n, source):
        ref, i = source
        up[k : k + n] = ref[i, NY - n : NY]
        dn[k : k + n] = ref[i, 0:n]

    for a in range(3):
        for m in range(ME):
            put(4 * (ME * a + m), 4, pick(m, low, u.at[a], high, (3 * a, 4 * a), ML))
        for m in range(ME - 2):
            source = pick(m, low, b.at[a], high, (9 + 2 * a, 12 + 3 * a), ML - 1)
            put(180 + 3 * (13 * a + m), 3, source)


def masked(x, n_low, flags, v, lo, hi):
    if flags is None:
        return v, lo, hi
    lo, hi = (lo * flags[2], hi * flags[3])
    if n_low <= x < n_low + NX:
        return v, lo, hi
    edge = flags[0] if x < n_low else flags[1]
    return v * edge, lo * edge, hi * edge


def fill(out, n, n_low, own, low, high, first, yl, yh, k, flags, rows):
    zero = jnp.zeros((8 - rows, NZ), F32)
    for x in range(n):
        ref, i = pick(x, low, own, high, first, n_low)
        j = k + rows * x
        v, lo, hi = masked(x, n_low, flags, ref[i], yl[j : j + rows], yh[j : j + rows])
        out[x, 0 : 8 - rows] = zero
        out[x, 8 - rows : 8] = lo
        out[x, 8:24] = v
        out[x, 24 : 24 + rows] = hi
        out[x, 24 + rows : 32] = zero


def fill_mech(out, n, n_low, own, low, high, first, yl, yh, k, flags, offset, rows):
    for x in range(n):
        ref, i = pick(x, low, own, high, first, n_low)
        j = k + rows * x
        lo, hi = yl[j : j + rows], yh[j : j + rows]
        v, lo, hi = masked(x, n_low, flags, ref[i], lo, hi)
        y = x + offset
        if rows < 4:
            out[y, 0 : 4 - rows] = jnp.zeros((4 - rows, NZ), F32)
            out[y, 20 + rows : 24] = jnp.zeros((4 - rows, NZ), F32)
        out[y, 4 - rows : 4] = lo
        out[y, 4:20] = v
        out[y, 20 : 20 + rows] = hi


def two_sum(a, b):
    s = a + b
    t = s - a
    return s, (a - (s - t)) + (b - t)


def halves(a):
    c = 4097.0 * a
    high = c - (c - a)
    return high, a - high


def two_product(a, b):
    p = a * b
    (ah, al), (bh, bl) = halves(a), halves(b)
    return p, ((ah * bh - p) + ah * bl + al * bh) + al * bl


def dot(pairs, start, rest):
    for a, b in pairs:
        p, e = two_product(a, b)
        start, f = two_sum(start, p)
        rest = rest + (e + f)
    return start, rest


def solve(m):
    def minus(a, b):
        d, e = two_sum(a[0], 0.0 - b[0])
        return d, e + (a[1] - b[1])

    g00, g01, g02 = m[1], m[2], m[3]
    g11, g12, g22 = minus(m[2], m[3]), minus(m[3], m[4]), minus(m[4], m[5])
    right = (m[0], m[1], minus(m[1], m[2]))
    inverse = lambda d, scale: jnp.where(d > PIVOT * jnp.abs(scale), 1.0 / d, 0.0)
    i0 = inverse(g00[0], 0.0 * g00[0])
    l10, l20 = g01[0] * i0, g02[0] * i0
    i1 = inverse(g11[0] - l10 * g01[0], g11[0])
    e = g12[0] - l10 * g02[0]
    l21 = e * i1
    i2 = inverse(g22[0] - l20 * g02[0] - l21 * e, g22[0])

    def eliminate(c0, c1, c2):
        c1 = c1 - l10 * c0
        c2 = c2 - l20 * c0 - l21 * c1
        y2 = c2 * i2
        y1 = c1 * i1 - l21 * y2
        return c0 * i0 - l10 * y1 - l20 * y2, y1, y2

    y = eliminate(*[r[0] for r in right])
    left = []
    for r, row in zip(right, ((g00, g01, g02), (g01, g11, g12), (g02, g12, g22))):
        rest = r[1]
        for a, v in zip(row, y):
            rest = rest - a[1] * v
        d, rest = dot([(a[0], 0.0 - v) for a, v in zip(row, y)], r[0], rest)
        left.append(d + rest)
    return [a + b for a, b in zip(y, eliminate(*left))]


def coefficients(rows):
    high, low = two_sum(rows[0:64], rows[64:128])
    while high.shape[0] > 8:
        n = high.shape[0] // 2
        rest = low[:n] + low[n:]
        high, low = two_sum(high[:n], high[n:])
        low = low + rest
    for n in (4, 2, 1):
        rest = low + pltpu.roll(low, n, 0)
        high, low = two_sum(high, pltpu.roll(high, n, 0))
        low = low + rest
    spread = lambda v, k: jnp.broadcast_to(v[:, k : k + 1], (8, 128))
    at = lambda k: (spread(high, k), spread(low, k))
    y = solve([at(k) for k in range(6)])
    y = (y[0] + y[1], y[2] - y[1], 0.0 - y[2])
    c = (jnp.ones((8, 128), F32), *y)
    weights = [c[a] * c[b] * (1.0 if a == b else 2.0) for a, b in PAIRS]
    mu = []
    for k in range(6):
        terms = [at(6 + 10 * k + i) for i in range(len(PAIRS))]
        rest = 0.0
        for w, t in zip(weights, terms):
            rest = rest + w * t[1]
        mu.append(dot([(w, t[0]) for w, t in zip(weights, terms)], 0.0 * y[0], rest))
    v = solve(mu)
    scalar = lambda x: x[0, 0]
    return [scalar(x) for x in y], [[scalar(x * c[g]) for g in range(GENS)] for x in v]


def differences(v, x, cx, cy, cz):
    c = v[x]
    fy, fz = cy[x] * (c - up_y(c)), cz[x] * (c - up_z(c))
    return (
        cx[x] * (c - v[x + 1])
        + cx[x - 1] * (c - v[x - 1])
        + (fy - dn_y(fy))
        + (fz - dn_z(fz))
    )


def pressure_chain(source, p, cx, cy, cz, inv, total, t, n, k, part):
    def first(x):
        r = source(x) - differences(p, x, cx, cy, cz)
        return [(n, (0, x), r), (t, (0, x), inv[x] * r)]

    loop(1, XE - 1, first, PW)
    for i in (1, 2):

        def follow(x):
            c = t[i - 1, x]
            a = total[x] * c + differences(t.at[i - 1], x, cx, cy, cz)
            d = inv[x] * a
            return [(n, (i, x), a), (k, (i - 1, x), d), (t, (i, x), c - d)]

        loop(1 + i, XE - 1 - i, follow, PW)

    def final(x):
        v = k[1, x]
        e = cx[x] * k[1, x + 1] + cy[x] * up_y(v) + cz[x] * up_z(v)
        return [(n, (3, x), 2.0 * e)]

    loop(LOW, LOW + NX, final, PW)

    def body(x, acc):
        s = [v[LOW + x, 8:24] for v in (t.at[0], k.at[0], k.at[1])]
        q = [n[i, LOW + x, 8:24] for i in range(4)]
        return tuple(v + s[i] * q[j] for v, (i, j) in zip(acc, LEVELS))

    sums = lax.fori_loop(0, NX, body, (jnp.zeros((NY, NZ), F32),) * 6)
    at = lax.broadcasted_iota(jnp.int32, (8, 128), 1)
    row = jnp.zeros((8, 128), F32)
    for k, v in enumerate(sums):
        row = jnp.where(at == k, jnp.sum(v), row)
    part[...] = row


def pressure_first_kernel(
    flags, mats, ids, p, f, low, high, yl, yh,
    code, pe, coef, t, part,
    fe, perm, stor, n, k,
):
    cx, cy, cz, inv, stab, base, biot, total = (coef.at[i] for i in range(8))
    fill(code, XE, LOW, ids, low, high, (0, 0), yl, yh, 0, flags, 6)
    fill(pe, XE, LOW, p, low, high, (6, 6), yl, yh, 120, flags, 6)
    fill(fe.at[1 : XE - 1], XE - 2, LOW - 1, f, low, high, (12, 12), yl, yh, 240, None, 5)

    def tables(x):
        l, s, k, st, bi = lookup(code[x], mats, range(5))
        bi = 0.25 * bi
        st2 = bi * bi / jnp.maximum(l + (2.0 / 3.0) * s, 1e-30)
        return [(perm, x, k), (stor, x, st), (biot, x, bi), (stab, x, st2)]

    loop(0, XE, tables)

    def faces(x):
        k = perm[x]

        def harmonic(other):
            return (2.0 * DT) * k * other / jnp.maximum(k + other, 1e-30)

        return [
            (cx, x, harmonic(perm[x + 1])),
            (cy, x, harmonic(up_y(k))),
            (cz, x, harmonic(up_z(k))),
        ]

    loop(0, XE - 1, faces, 2)

    def diagonal(x):
        y, z = cy[x], cz[x]
        flow = cx[x] + cx[x - 1] + y + dn_y(y) + z + dn_z(z)
        inside = code[x] > 0.5
        d = stor[x] + stab[x] + flow
        return [
            (inv, x, jnp.where(inside, 1.0 / jnp.where(inside, d, 1.0), 0.0)),
            (total, x, stor[x] + stab[x]),
            (base, x, stor[x] * pe[x] + DT * fe[x]),
        ]

    loop(1, XE - 1, diagonal, 2)
    pressure_chain(lambda x: DT * fe[x], pe, cx, cy, cz, inv, total, t, n, k, part)


def pressure_next_kernel(
    flags, coef, p, du, uo, low, high, yl, yh,
    pe, ue, t, part,
    de, n, k,
):
    cx, cy, cz, inv, stab, base, biot, total = (coef.at[i] for i in range(8))
    edge = lambda x, n: flags[0] if x < n else flags[1]
    zero = jnp.zeros((2, NZ), F32)
    for a in range(3):
        for x in range(19):
            j = 6 * (19 * a + x)
            out = de.at[a, x + 1]
            lo, hi = yl[j : j + 6] * flags[2], yh[j : j + 6] * flags[3]
            if 5 <= x < 14:
                out[4:28] = du[a, x - 5]
            else:
                outer = edge(x, 5)
                lo, hi = lo * outer, hi * outer
                ref = low.at[5 * a + x] if x < 5 else high.at[5 * a + x - 14]
                out[8:24] = ref[...] * outer
            if x == 13:
                lo, hi = lo * flags[1], hi * flags[1]
            out[0:2] = zero
            out[2:8] = lo
            out[24:30] = hi
            out[30:32] = zero
    for x in range(XE):
        j = 342 + 6 * x
        lo, hi = yl[j : j + 6] * flags[2], yh[j : j + 6] * flags[3]
        if not LOW <= x < LOW + NX:
            lo, hi = lo * edge(x, LOW), hi * edge(x, LOW)
        if 3 <= x < 17:
            pe[x, 8:24] = p[x - 3, 8:24]
        else:
            ref = low.at[15 + x] if x < 3 else high.at[15 + x - 17]
            pe[x, 8:24] = ref[...] * edge(x, LOW)
        pe[x, 0:2] = zero
        pe[x, 2:8] = lo
        pe[x, 24:30] = hi
        pe[x, 30:32] = zero

    def start(x):
        c2 = de[2, x]
        div = (
            (de[0, x + 1] - de[0, x])
            + (up_y(de[1, x]) - de[1, x])
            + (up_z(c2) - c2)
        )
        return base[x] - biot[x] * div + (stab[x] - total[x]) * pe[x]

    pressure_chain(start, pe, cx, cy, cz, inv, total, t, n, k, part)
    for a in range(3):
        for m in range(ME):
            ue[a, m] = uo[a, m] + de[a, m + MO, 4:28]


def mech_chain(u, bf, pe, t, biot, mc, kept, q, load, carry, acc, s, tg, part_p, part):
    sx, sy, sz, half, lame, h0, h1, h2, kk = (mc.at[i] for i in range(9))
    h = (h0, h1, h2)

    def loads(m):
        x = m + MO
        bi = biot[x, 4:28]
        fields = [pe[x, 4:28]] + [t[i, x, 4:28] for i in range(3)]
        return [(load, (g, m), bi * v) for g, v in enumerate(fields)]

    loop(0, ME - 1, loads, 2)

    def precondition(r, m):
        hs = [h[a][m] for a in range(3)]
        scaled = [r[a] * hs[a] for a in range(3)]
        k = kk[m] * (scaled[0] + scaled[1] + scaled[2])
        return [scaled[a] - hs[a] * k for a in range(3)]

    def apply(w, m, more, below):
        c = [w[a, m] for a in range(3)]
        d = (c[0] - w[0, m + 1], c[1] - up_y(c[1]), c[2] - up_z(c[2]))
        l = 0.0 - lame[m] * (d[0] + d[1] + d[2])
        if more is not None:
            l = l - more
        x, xb, y, z, g = sx[m], sx[m - 1], sy[m], sz[m], half[m, :, :128]

        def along_x(a):
            return x * (c[a] - w[a, m + 1]) + xb * (c[a] - w[a, m - 1])

        def along_y(a):
            f = y * (c[a] - up_y(c[a]))
            return f - dn_y(f)

        def along_z(a):
            f = z * (c[a] - up_z(c[a]))
            return f + dn_z(0.0 - f, g * c[a][:, :128])

        fx, fy, fz = x * d[0], y * d[1], z * d[2]
        r = [
            (fx + below - l) + along_y(0) + along_z(0),
            (fy + dn_y(l - fy) - l) + along_x(1) + along_z(1),
            (fz + dn_z(l - fz, g * c[2][:, :128]) - l) + along_x(2) + along_y(2),
        ]
        return r, l - fx

    def carried(w, m, more):
        c = [w[a, m] for a in range(3)]
        d = (c[0] - w[0, m + 1], c[1] - up_y(c[1]), c[2] - up_z(c[2]))
        l = 0.0 - lame[m] * (d[0] + d[1] + d[2])
        if more is not None:
            l = l - more
        return l - sx[m] * d[0]

    carry[0] = carried(u, 0, load[0, 0])

    def own(m):
        return jnp.where((m >= ML) & (m < ML + NX), m - ML, NX)

    def near(m):
        return jnp.where((m >= ML) & (m <= ML + NX), m - ML, NX + 1)

    def residual(m):
        for g in range(GENS):
            if g == 0:
                r, up = apply(u, m, load[0, m], carry[0])
                yield carry, 0, up
                r = [bf[a, m] - r[a] for a in range(3)]
            else:
                c = load[g, m]
                r = [load[g, m - 1] - c, dn_y(c) - c, dn_z(c) - c]
            z = precondition(r, m)
            for a in range(3):
                yield q, (0, g, a, own(m)), r[a]
                yield s, (0, g, a, m), z[a]
                yield kept, (g * 3 + a, near(m)), z[a]

    loop(1, ME - 1, residual, 2)

    for i in (1, 2):
        for g in range(GENS):
            carry[g] = carried(s.at[i - 1, g], i, None)

        def follow(m):
            for g in range(GENS):
                w = s.at[i - 1, g]
                r, up = apply(w, m, None, carry[g])
                yield carry, g, up
                v = precondition(r, m)
                for a in range(3):
                    yield q, (i, g, a, own(m)), r[a]
                    yield kept, ((i * GENS + g) * 3 + a, near(m)), v[a]
                    if i == 1:
                        yield s, (1, g, a, m), w[a, m] - v[a]

        loop(1 + i, ME - 1 - i, follow)

    def energy(m):
        l, x, y, z = lame[m], sx[m], sy[m], sz[m]
        low = (0.5 * lame[m - 1], 0.5 * dn_y(l), 0.5 * dn_z(l))
        for g in range(GENS):
            k = (2 * GENS + g) * 3
            w, o = kept.at[k : k + 3], ML
            total = 0.0
            for a in range(3):
                c = w[a, m - o]
                up = (w[a, m + 1 - o], up_y(c), up_z(c))
                total = total + up[a]
                yield q, (3, g, a, m - ML), x * up[0] + y * up[1] + z * up[2] + low[a] * c
            near_sum = w[0, m - o] + w[1, m - o] + w[2, m - o]
            yield tg, (0, g, m - ML), total
            yield tg, (1, g, m - ML), l * (near_sum - 0.5 * total)

    loop(ML, ML + NX, energy)

    top = lax.broadcasted_iota(jnp.int32, (8, NZ), 0) >= 4
    for k, (i, j) in enumerate(LEVELS):

        def body(step, sums):
            sums = list(sums)
            for x in (2 * step, 2 * step + 1):
                for a in range(3 if j < 3 else 4):
                    if a < 3:
                        v = [kept[(i * GENS + g) * 3 + a, x] for g in range(GENS)]
                        w = [q[j, g, a, x] for g in range(GENS)]
                    else:
                        v = [tg[0, g, x] for g in range(GENS)]
                        w = [tg[1, g, x] for g in range(GENS)]
                    for pick_rows in (
                        lambda f: f[8:16],
                        lambda f: jnp.where(top, f[0:8], f[16:24]),
                    ):
                        vt, wt = [pick_rows(f) for f in v], [pick_rows(f) for f in w]
                        sums = [c + vt[g] * wt[o] for c, (g, o) in zip(sums, PAIRS)]
                        if j == 3:
                            sums = [c + vt[o] * wt[g] for c, (g, o) in zip(sums, PAIRS)]
            return tuple(sums)

        sums = lax.fori_loop(0, NX // 2, body, (jnp.zeros((8, NZ), F32),) * len(PAIRS))
        for n, v in enumerate(sums):
            acc[10 * k + n] = v
    at = lax.broadcasted_iota(jnp.int32, (8, 128), 1)
    row = part_p[...]
    for k in range(60):
        row = jnp.where(at == k + 6, jnp.sum(acc[k]), row)
    for i in range(0, 128, 8):
        part[i : i + 8] = row


def mech_first_kernel(
    flags, mats, part_p, code, pe, coef, t, u, b, low, high, yl, yh,
    ue, be, mc, kept, part,
    q, load, shear, carry, acc, s, tg,
):
    sx, sy, sz, half, lame, h0, h1, h2, kk = (mc.at[i] for i in range(9))
    for a in range(3):
        fill_mech(ue.at[a], ME, ML, u.at[a], low, high, (3 * a, 4 * a), yl, yh, 60 * a, flags, 0, 4)
        fill_mech(
            be.at[a], ME - 2, ML - 1, b.at[a], low, high, (9 + 2 * a, 12 + 3 * a), yl, yh, 180 + 39 * a, None, 1, 3
        )

    def tables(m):
        l, g = lookup(code[m + MO, 4:28], mats, (0, 1))
        return [(lame, m, l), (shear, m, g)]

    loop(0, ME, tables)

    def faces(m):
        g = shear[m]
        return [
            (sx, m, 0.5 * (g + shear[m + 1])),
            (sy, m, 0.5 * (g + up_y(g))),
            (sz, m, 0.5 * (g + up_z(g))),
        ]

    loop(0, ME - 1, faces, 2)

    def diagonal(m):
        g, l = shear[m], lame[m]
        near = (
            shear[m + 1] + shear[m - 1] + up_y(g) + dn_y(g)
            + up_z(g) + dn_z(g)
        )
        d = 3.0 * g + 0.5 * near
        inside = g > 0.0
        lows = (lame[m - 1], dn_y(l), dn_z(l))
        hs = [jnp.where(inside, 1.0 / jnp.where(inside, d + v, 1.0), 0.0) for v in lows]
        k = l / (1.0 + l * (hs[0] + hs[1] + hs[2]))
        return [(half, m, 0.5 * g), (h0, m, hs[0]), (h1, m, hs[1]), (h2, m, hs[2]), (kk, m, k)]

    loop(1, ME - 1, diagonal, 2)
    mech_chain(ue, be, pe, t, coef.at[6], mc, kept, q, load, carry, acc, s, tg, part_p, part)


def mech_next_kernel(
    part_p, pe, coef, t, ue, be, mc,
    kept, part,
    q, load, carry, acc, s, tg,
):
    mech_chain(ue, be, pe, t, coef.at[6], mc, kept, q, load, carry, acc, s, tg, part_p, part)


def combine(v, kept, a, x):
    total = 0.0
    for i in range(3):
        for g in range(GENS):
            total = total + v[i][g] * kept[(i * GENS + g) * 3 + a, x]
    return total


def change_kernel(rows, t, pe, kept, u, du, pnew, unew, up, dn):
    y, v = coefficients(rows)
    for k in range(PK):
        x = k + MO
        w = pe[x] + (y[0] * t[0, x] + y[1] * t[1, x] + y[2] * t[2, x])
        pnew[k] = w
        i = k - ML
        if 2 <= i <= 4:
            up[13 + i] = w[8:24]
        if 3 <= i <= 5:
            dn[12 + i] = w[8:24]
    for a in range(3):
        for i in range(NX + 1):
            d = combine(v, kept, a, i)
            du[a, i] = d
            if i < NX:
                unew[a, i] = u[a, i] + d[4:20]
            if 3 <= i <= 7:
                up[5 * a + i - 3] = d[4:20]
            if 1 <= i <= 5:
                dn[5 * a + i - 1] = d[4:20]


def pack_change_kernel(du, p, low, high, up, dn):
    for a in range(3):
        for x in range(19):
            if x < 5:
                ref, r = low.at[5 * a + x], 0
            elif x < 14:
                ref, r = du.at[a, x - 5], 4
            else:
                ref, r = high.at[5 * a + x - 14], 0
            k = 6 * (19 * a + x)
            up[k : k + 6] = ref[r + 10 : r + 16]
            dn[k : k + 6] = ref[r : r + 6]
    for x in range(XE):
        if x < 3:
            ref, r = low.at[15 + x], 0
        elif x < 17:
            ref, r = p.at[x - 3], 8
        else:
            ref, r = high.at[15 + x - 17], 0
        k = 342 + 6 * x
        up[k : k + 6] = ref[r + 10 : r + 16]
        dn[k : k + 6] = ref[r : r + 6]


def finish_kernel(rows, t, p, kept, u, unew, pnew):
    y, v = coefficients(rows)
    for x in range(NX):
        k = x + LOW
        w = p[k, 8:24] + (y[0] * t[0, k, 8:24] + y[1] * t[1, k, 8:24] + y[2] * t[2, k, 8:24])
        pnew[x] = w
        for a in range(3):
            unew[a, x] = u[a, x] + combine(v, kept, a, x)[4:20]


def call(kernel, name, ins, outs, scratch=(), specs=None, cost=0, limit=12):
    return pl.pallas_call(
        kernel,
        name=name,
        out_shape=[jax.ShapeDtypeStruct(o, F32) for o in outs],
        in_specs=specs or [VM] * len(ins),
        out_specs=[VM] * len(outs),
        scratch_shapes=[pltpu.VMEM(s, F32) if isinstance(s, tuple) else s for s in scratch],
        compiler_params=pltpu.CompilerParams(vmem_limit_bytes=limit * 2**20),
        cost_estimate=pl.CostEstimate(flops=cost, bytes_accessed=0, transcendentals=0) if cost else None,
    )(*ins)


def neighbours(axis, size, up, dn):
    ring = [(i, (i + 1) % size) for i in range(size)]
    return lax.ppermute(up, axis, ring), lax.ppermute(dn, axis, [(b, a) for a, b in ring])


def gather_rows(part):
    return lax.all_to_all(part, ("gx", "gy"), 0, 0, tiled=True)


def on_device(gx_size, gy_size, u, p, b, f, ids, mats):
    gx, gy = lax.axis_index("gx"), lax.axis_index("gy")
    flags = jnp.stack([gx > 0, gx < gx_size - 1, gy > 0, gy < gy_size - 1]).astype(F32)
    wide, mech = (YE, NZ), (YM, NZ)
    in_hbm = lambda v: pltpu.with_memory_space_constraint(v, pltpu.HBM)
    up_p, dn_p, own_code, own_p, own_f = call(
        pack_x_pressure_kernel,
        "pack_xp",
        [in_hbm(v) for v in (ids, p, f)],
        [(17, NY, NZ)] * 2 + [(NX, NY, NZ)] * 3,
        [pltpu.VMEM((NX, NY, NZ), jnp.int32), pltpu.SemaphoreType.DMA((7,))],
        [HB] * 3,
    )
    up_m, dn_m = call(
        pack_x_mech_kernel,
        "pack_xm",
        (in_hbm(u), in_hbm(b), own_code),
        [(15, NY, NZ), (21, NY, NZ)],
        [pltpu.SemaphoreType.DMA((12,))],
        [HB, HB, pl.BlockSpec(memory_space=pl.ANY)],
    )
    low_p, high_p = neighbours("gx", gx_size, up_p, dn_p)
    low_m, high_m = neighbours("gx", gx_size, up_m, dn_m)
    up, dn = call(
        pack_y_pressure_kernel, "pack_yp", (own_code, own_p, own_f, low_p, high_p), [(336, NZ), (336, NZ)], limit=4
    )
    yl_p, yh_p = neighbours("gy", gy_size, up, dn)
    up, dn = call(pack_y_mech_kernel, "pack_ym", (u, b, low_m, high_m), [(304, NZ), (304, NZ)], limit=4)
    yl_m, yh_m = neighbours("gy", gy_size, up, dn)
    code, pe, coef, t, part_p = call(
        pressure_first_kernel,
        "pressure_first",
        (flags, mats, own_code, own_p, own_f, low_p, high_p, yl_p, yh_p),
        [(XE, *wide), (XE, *wide), (8, XE, *wide), (3, XE, *wide), (8, 128)],
        [(XE, *wide)] * 3 + [(4, XE, *wide), (2, XE, *wide)],
        [SM, SM] + [VM] * 7,
        2_000_000_000,
    )
    mech_scratch = [
        (4, GENS, 3, NX + 1, *mech),
        (GENS, ME, *mech),
        (GENS, *mech),
        (60, 8, NZ),
        (2, GENS, 3, ME, *mech),
        (2, GENS, NX, *mech),
    ]
    basis = (9 * GENS, NX + 2, *mech)
    ue, be, mc, s, part = call(
        mech_first_kernel,
        "mech_first",
        (flags, mats, part_p, code, pe, coef, t, u, b, low_m, high_m, yl_m, yh_m),
        [(3, ME, *mech), (3, ME, *mech), (9, ME, *mech), basis, (128, 128)],
        mech_scratch[:2] + [(ME, *mech)] + mech_scratch[2:],
        [SM, SM] + [VM] * 11,
        COST,
        26,
    )
    rows = gather_rows(part)
    du, p1, u1, up, dn = call(
        change_kernel,
        "change",
        (rows, t, pe, s, u),
        [(3, NX + 1, *mech), (PK, *wide), (3, NX, NY, NZ), (18, NY, NZ), (18, NY, NZ)],
    )
    low, high = neighbours("gx", gx_size, up, dn)
    up, dn = call(pack_change_kernel, "pack_change", (du, p1, low, high), [(464, NZ), (464, NZ)])
    yl, yh = neighbours("gy", gy_size, up, dn)
    pe, ue, t, part_p = call(
        pressure_next_kernel,
        "pressure_next",
        (flags, coef, p1, du, ue, low, high, yl, yh),
        [(XE, *wide), (3, ME, *mech), (3, XE, *wide), (8, 128)],
        [(3, XE, *wide), (4, XE, *wide), (2, XE, *wide)],
        [SM] + [VM] * 8,
        COST,
    )
    s, part = call(
        mech_next_kernel,
        "mech_next",
        (part_p, pe, coef, t, ue, be, mc),
        [basis, (128, 128)],
        mech_scratch,
        None,
        COST,
        26,
    )
    rows = gather_rows(part)
    u2, p2 = call(
        finish_kernel,
        "finish",
        (rows, t, pe, s, u1),
        [(3, NX, NY, NZ), (NX, NY, NZ)],
    )
    return u2, p2


def solution(mesh):
    body = functools.partial(on_device, mesh.shape["gx"], mesh.shape["gy"])
    field, vector = P("gx", "gy", None), P(None, "gx", "gy", None)
    return jax.shard_map(
        body,
        mesh=mesh,
        in_specs=(vector, field, vector, field, field, P()),
        out_specs=(vector, field),
        check_vma=False,
    )
```
